256 devices in a mesh: lat: 16 (over y, x), lon: 16 (over z, core).
Axes of the slice: x: 4, y: 4, z: 8, core: 2. Of those that a mesh axis runs over, the one named last changes fastest.
Arguments:
- fine_nodes: float32 [2, 512, 512, 512], P(None, 'lat', 'lon'), may hold values from -6 to 6
- mid_nodes: float32 [2, 128, 128, 512], P(None, 'lat', 'lon'), may hold values from -6 to 6
- coarse_nodes: float32 [2, 32, 32, 512], P(None, 'lat', 'lon'), may hold values from -6 to 6
- edge_flags: int32 [8, 512, 512], P(None, 'lat', 'lon'), may hold values 0 or 1
- proc_weights: bfloat16 [3, 4, 512, 512], replicated, may hold values from -0.25 to 0.25
- bridge_weights: bfloat16 [4, 512, 512], replicated, may hold values from -0.25 to 0.25
- proc_biases: float32 [3, 512], replicated, may hold values from -3 to 3
Outputs:
- refined: float32 [2, 512, 512, 512], P(None, 'lat', 'lon')
- fine_average: bfloat16 [2, 512, 512, 512], P(None, 'lat', 'lon')
The draws below stay inside these ranges and needn't reach their ends.
All inputs are finite; a program needn't handle non-finite values. No bound on the sum of `edge_flags` on one device may be relied on, other than what follows from the above.
Results may differ from the reference program's by a relative error of at most 0.005.
Values may be sent and summed in bfloat16 or wider, within the bound.
No kernel may reach another device: no remote copies, remote signals or barrier semaphores. Data moves between devices by JAX's collectives and lax.ppermute only.
A program may use at most 128 MiB of HBM per device.

```python
import jax
import jax.numpy as jnp
from jax import lax

D = 512
SAMPLES = 2
NF_LAT = 512
NF_LON = 512
NM_LAT = 128
NM_LON = 128
NC_LAT = 32
NC_LON = 32


def with_ends(values, rng, least, high):
    place = [jax.random.randint(jax.random.fold_in(rng, axis), (), 0, length) for axis, length in enumerate(values.shape)]
    longest = values.shape.index(max(values.shape))
    beside = place[:longest] + [(place[longest] + 1) % values.shape[longest]] + place[longest + 1:]
    return values.at[tuple(place)].set(least).at[tuple(beside)].set(high)


def block_scale(rng, shape, shards, smallest, top_value):
    level = 1.0
    for position, blocks in shards:
        draws = jax.random.uniform(jax.random.fold_in(jax.random.fold_in(rng, 6), position), (blocks,), jnp.float32, smallest / len(shards), top_value / len(shards))
        level = level * jnp.repeat(jnp.exp(draws), shape[position] // blocks).reshape((-1,) + (1,) * (len(shape) - 1 - position))
    return level


def scatter_about(key, dims, scale, reach, split=(), dtype=jnp.bfloat16):
    level = block_scale(key, dims, split, -0.22, 0.18) if split else 1.0
    values = jax.random.normal(key, dims, jnp.float32) * scale * level
    return jnp.minimum(jnp.maximum(values, -reach), reach).astype(dtype)


def setup_inputs(seed: int = 0) -> dict:
    keys = jax.random.split(jax.random.key(seed), 8)
    return {
        "fine_nodes": scatter_about(keys[0], (SAMPLES, NF_LAT, NF_LON, D), 1.0, 6.0, ((1, 16), (2, 16)), jnp.float32),
        "mid_nodes": scatter_about(keys[1], (SAMPLES, NM_LAT, NM_LON, D), 1.0, 6.0, ((1, 16), (2, 16)), jnp.float32),
        "coarse_nodes": scatter_about(keys[2], (SAMPLES, NC_LAT, NC_LON, D), 1.0, 6.0, ((1, 16), (2, 16)), jnp.float32),
        "edge_flags": with_ends((jax.random.randint(keys[3], (8, NF_LAT, NF_LON), 0, 8) < 7).astype(jnp.int32), jax.random.fold_in(keys[3], 1), 0, 1),
        "proc_weights": scatter_about(keys[4], (3, 4, D, D), D ** -0.5, 0.25),
        "bridge_weights": scatter_about(keys[5], (4, D, D), D ** -0.5, 0.25),
        "proc_biases": scatter_about(keys[6], (3, D), 0.5, 3.0, (), jnp.float32),
    }


offsets = ((-1, -1), (-1, 0), (-1, 1), (0, -1), (0, 1), (1, -1), (1, 0), (1, 1))


def neighbour(values, step_lat, step_lon):
    rows = values.shape[0]
    padded = jnp.pad(values, ((1, 1), (0, 0), (0, 0)))
    shifted = padded[1 + step_lat:1 + step_lat + rows]
    return jnp.roll(shifted, -step_lon, axis=1)


def project(values, matrix):
    shape = values.shape
    flat = values.reshape(-1, shape[-1])
    result = jnp.dot(flat, matrix, preferred_element_type=jnp.float32)
    return result.reshape(shape[:-1] + (matrix.shape[1],))


def level_pass(states, flag_grid, weights, biases):
    rows = states.shape[0]
    operand = states.astype(jnp.bfloat16)
    receiver = project(operand, weights[0])
    sender = project(operand, weights[1]).astype(jnp.bfloat16)
    row_ids = jnp.arange(rows)
    summed = jnp.zeros(states.shape, jnp.float32)
    for direction, (step_lat, step_lon) in enumerate(offsets):
        inside = ((row_ids + step_lat >= 0) & (row_ids + step_lat < rows)).astype(jnp.float32)[:, None]
        if flag_grid is None:
            usable = inside
        else:
            usable = inside * flag_grid[direction].astype(jnp.float32)
        nearby = neighbour(sender, step_lat, step_lon).astype(jnp.float32)
        hidden = jax.nn.silu(receiver + nearby + biases).astype(jnp.bfloat16)
        message = jax.nn.silu(project(hidden, weights[2]))
        summed = summed + usable[:, :, None] * message
    average = (summed * 0.125).astype(jnp.bfloat16)
    return states + project(average, weights[3]), average


def pooled(states):
    rows, cols, features = states.shape
    blocks = states.reshape(rows // 4, 4, cols // 4, 4, features)
    return jnp.mean(blocks, axis=(1, 3)).astype(jnp.bfloat16)


def expand(values):
    return jnp.repeat(jnp.repeat(values, 4, axis=0), 4, axis=1)


def reference(fine_nodes, mid_nodes, coarse_nodes, edge_flags, proc_weights, bridge_weights, proc_biases):
    def single(packed):
        fine_state, mid_state, coarse_state = packed
        fine_one, fine_average = level_pass(fine_state, edge_flags, proc_weights[0], proc_biases[0])
        mid_zero = mid_state + jax.nn.silu(project(pooled(fine_one), bridge_weights[0]))
        mid_one, unused_mid = level_pass(mid_zero, None, proc_weights[1], proc_biases[1])
        coarse_zero = coarse_state + jax.nn.silu(project(pooled(mid_one), bridge_weights[1]))
        coarse_one, unused_coarse = level_pass(coarse_zero, None, proc_weights[2], proc_biases[2])
        lifted = jax.nn.silu(project(coarse_one.astype(jnp.bfloat16), bridge_weights[2]))
        mid_two = mid_one + expand(lifted)
        spread = jax.nn.silu(project(mid_two.astype(jnp.bfloat16), bridge_weights[3]))
        return fine_one + expand(spread), fine_average

    return lax.map(single, (fine_nodes, mid_nodes, coarse_nodes))
```

```python
import functools
import jax
import jax.numpy as jnp
import numpy as np
from jax import lax
from jax.experimental import pallas as pl
from jax.experimental.pallas import tpu as pltpu
from jax.sharding import PartitionSpec as P

D = 512
BF = jnp.bfloat16
F32 = jnp.float32
OFFS = ((-1, -1), (-1, 0), (-1, 1), (0, -1), (0, 1), (1, -1), (1, 0), (1, 1))
PRB = 8
RB = 8


def mm(a, b):
    return jnp.dot(a, b, preferred_element_type=F32)


def gate(half):
    return half + half * jnp.tanh(half)


def pool_rows(x, g, tmp):
    tall = (x[4 * g] + x[4 * g + 1]) + (x[4 * g + 2] + x[4 * g + 3])
    parts = []
    for lane in range(4):
        tmp[g, lane] = tall[:, lane * 128:(lane + 1) * 128]
        part = tmp[g, lane, pl.ds(0, 8, stride=4), :]
        for t in range(1, 4):
            part = part + tmp[g, lane, pl.ds(t, 8, stride=4), :]
        parts.append(part)
    return jnp.concatenate(parts, axis=1)


def prep_kernel(s_ref, w_ref, c_ref, r_out, t_out, ps_out, tmp):
    x = s_ref[0]
    op = x.reshape(PRB * 32, D).astype(BF)
    r = mm(op, w_ref[0, 0])
    r_out[0] = (0.5 * (r + c_ref[0:1, :])).astype(BF).reshape(PRB, 32, D)
    t_out[0] = (0.5 * mm(op, w_ref[0, 1])).astype(BF).reshape(PRB, 32, D)
    for g in range(PRB // 4):
        ps_out[0, g] = pool_rows(x, g, tmp)


def prep(fine, pw, pb):
    return pl.pallas_call(
        prep_kernel,
        name="prep",
        grid=(2, 32 // PRB),
        in_specs=[
            pl.BlockSpec((1, PRB, 32, D), lambda b, i: (b, i, 0, 0)),
            pl.BlockSpec((1, 2, D, D), lambda b, i: (0, 0, 0, 0)),
            pl.BlockSpec((3, D), lambda b, i: (0, 0)),
        ],
        out_specs=[
            pl.BlockSpec((1, PRB, 32, D), lambda b, i: (b, i, 0, 0)),
            pl.BlockSpec((1, PRB, 32, D), lambda b, i: (b, i, 0, 0)),
            pl.BlockSpec((1, PRB // 4, 8, D), lambda b, i: (b, i, 0, 0)),
        ],
        out_shape=[
            jax.ShapeDtypeStruct((2, 32, 32, D), BF),
            jax.ShapeDtypeStruct((2, 32, 32, D), BF),
            jax.ShapeDtypeStruct((2, 8, 8, D), F32),
        ],
        scratch_shapes=[pltpu.VMEM((8, 4, 32, 128), F32)],
        compiler_params=pltpu.CompilerParams(vmem_limit_bytes=32 << 20),
        cost_estimate=pl.CostEstimate(flops=2 * 2 * 2048 * D * D, bytes_accessed=10 << 20, transcendentals=0),
    )(fine, pw, pb)


def stack_rows(parts, shape):
    rows = lax.broadcasted_iota(jnp.int32, shape, 0)
    out = jnp.zeros(shape, F32)
    for i, part in enumerate(parts):
        out = jnp.where(rows == i, jnp.broadcast_to(part.astype(F32), shape), out)
    return out


def edge_kernel(r_ref, t_ref, up_ref, down_ref, left_ref, right_ref, ul_ref, ur_ref, dl_ref, dr_ref,
                mask_ref, w_ref, b0_ref, ps_ref, mid_ref, pick_ref,
                avg_out, mz_out, *rest):
    rim_outs, (sh, hs, tmp, pa) = rest[:8], rest[8:]
    b = pl.program_id(0)
    blk = pl.program_id(1)

    @pl.when(blk == 0)
    def _():
        rim = jnp.concatenate([up_ref[0], down_ref[0], left_ref[0], right_ref[0]], axis=0)
        hs[0:128, :] = (0.5 * mm(rim, w_ref[0, 1])).astype(BF).astype(F32)
        corners = stack_rows([ul_ref[0], ur_ref[0], dl_ref[0], dr_ref[0]], (8, D)).astype(BF)
        hs[128:136, :] = (0.5 * mm(corners, w_ref[0, 1])).astype(BF).astype(F32)
        rows = lax.broadcasted_iota(jnp.int32, (32, D), 0)

        def put(i, x, left, right):
            sh[1, i] = x.astype(BF)
            sh[0, i] = jnp.where(rows == 0, jnp.broadcast_to(left, (32, D)), pltpu.roll(x, 1, 0)).astype(BF)
            sh[2, i] = jnp.where(rows == 31, jnp.broadcast_to(right, (32, D)), pltpu.roll(x, 31, 0)).astype(BF)

        put(0, hs[0:32, :], hs[128:129, :], hs[129:130, :])
        put(33, hs[32:64, :], hs[130:131, :], hs[131:132, :])

        @pl.loop(0, 32)
        def _(i):
            put(i + 1, t_ref[0, i].astype(F32), hs[pl.ds(64 + i, 1), :], hs[pl.ds(96 + i, 1), :])

    row0 = blk * RB
    rv = r_ref[0].reshape(RB * 32, D)
    acc = None
    for k, (p, q) in enumerate(OFFS):
        sv = sh[q + 1, pl.ds(row0 + 1 + p, RB)].reshape(RB * 32, D)
        x = rv + sv
        m = mask_ref[k].reshape(RB * 32, 128)
        h = gate(x) * jnp.concatenate([m] * 4, axis=1)
        g = 0.5 * mm(h, w_ref[0, 2])
        msg = gate(g)
        acc = msg if acc is None else acc + msg
    avg = (acc * 0.125).astype(BF)
    av = avg.reshape(RB, 32, D)
    avg_out[0] = av
    af = av.astype(F32)
    for g in range(RB // 4):
        pa[b, blk * (RB // 4) + g] = pool_rows(af, g, tmp)

    @pl.when((b == 1) & (blk == 32 // RB - 1))
    def _():
        mean_avg = (pa[...].reshape(128, D) * 0.0625).astype(BF)
        pooled = (ps_ref[...].reshape(128, D) * 0.0625 + mm(mean_avg, w_ref[0, 3])).astype(BF)
        mz = mid_ref[...].reshape(128, D) + gate(0.5 * mm(pooled, b0_ref[0]))
        mz_out[...] = mz
        rims = mm(pick_ref[...], mz.astype(BF)).astype(BF)
        for d in range(8):
            rim_outs[d][...] = rims[16 * d:16 * d + 16]


def edge(r, t, rim, mask, pw, bw, ps, mid, pick):
    whole = lambda *shape: pl.BlockSpec(shape, lambda b, i: (0,) * len(shape))
    return pl.pallas_call(
        edge_kernel,
        name="edge",
        grid=(2, 32 // RB),
        in_specs=[
            pl.BlockSpec((1, RB, 32, D), lambda b, i: (b, i, 0, 0)),
            pl.BlockSpec((1, 32, 32, D), lambda b, i: (b, 0, 0, 0)),
        ]
        + [pl.BlockSpec((1, 32, D), lambda b, i: (b, 0, 0))] * 4
        + [pl.BlockSpec((1, 1, D), lambda b, i: (b, 0, 0))] * 4
        + [
            pl.BlockSpec((8, RB, 32, 128), lambda b, i: (0, i, 0, 0)),
            whole(1, 4, D, D),
            whole(1, D, D),
            whole(2, 8, 8, D),
            whole(2, 8, 8, D),
            whole(128, 128),
        ],
        out_specs=[
            pl.BlockSpec((1, RB, 32, D), lambda b, i: (b, i, 0, 0)),
            whole(128, D),
        ]
        + [whole(16, D)] * 8,
        out_shape=[
            jax.ShapeDtypeStruct((2, 32, 32, D), BF),
            jax.ShapeDtypeStruct((128, D), F32),
        ]
        + [jax.ShapeDtypeStruct((16, D), BF)] * 8,
        scratch_shapes=[
            pltpu.VMEM((3, 34, 32, D), BF),
            pltpu.VMEM((136, D), F32),
            pltpu.VMEM((8, 4, 32, 128), F32),
            pltpu.VMEM((2, 8, 8, D), F32),
        ],
        compiler_params=pltpu.CompilerParams(vmem_limit_bytes=48 << 20),
        cost_estimate=pl.CostEstimate(flops=2 * 8 * 2048 * D * D, bytes_accessed=16 << 20, transcendentals=16 << 20),
    )(r, t, *rim, mask, pw, bw, ps, mid, pick)


def middle_kernel(inner_ref, mz_ref, *refs):
    rim_refs = refs[:8]
    w_ref, c_ref, b1_ref, coarse_ref, gather_ref, mean_ref, mo_out, cz_out, czb_out = refs[8:]
    mz = mz_ref[...]
    own = mz.astype(BF)
    recv = 0.5 * (mm(own, w_ref[0, 0]) + c_ref[1:2, :])
    states = jnp.concatenate([own] + [ref[...] for ref in rim_refs], axis=0)
    send = (0.5 * mm(states, w_ref[0, 1])).astype(BF)
    near = mm(gather_ref[...], send)
    hidden = gate(near.reshape(8, 128, D) + recv[None]).astype(BF).reshape(1024, D)
    msg = gate(0.5 * mm(hidden, w_ref[0, 2])).reshape(8, 128, D)
    lat = (lax.broadcasted_iota(jnp.int32, (128, D), 0) // 8) % 8
    up = jnp.where(lat == 0, inner_ref[0], 1.0)
    down = jnp.where(lat == 7, inner_ref[1], 1.0)
    total = up * (msg[0] + msg[1] + msg[2]) + (msg[3] + msg[4]) + down * (msg[5] + msg[6] + msg[7])
    avg = (0.125 * total).astype(BF)
    mo = mz + mm(avg, w_ref[0, 3])
    mo_out[...] = mo
    pooled = jnp.dot(mean_ref[...], mo, preferred_element_type=F32, precision=lax.Precision.HIGHEST)
    cz = coarse_ref[...] + gate(0.5 * mm(pooled.astype(BF), b1_ref[0]))
    cz_out[...] = cz
    czb_out[...] = cz.astype(BF)


VM = pl.BlockSpec(memory_space=pltpu.VMEM)


def level_block(level):
    return pl.BlockSpec((1, 4, D, D), lambda i: (level, 0, 0, 0))


def bridge_block(index):
    return pl.BlockSpec((1, D, D), lambda i: (index, 0, 0))


def full(*shape):
    return pl.BlockSpec(shape, lambda i: (0,) * len(shape))


def middle(inner, mz, rim, pw, pb, bw, coarse, gather, mean):
    return pl.pallas_call(
        middle_kernel,
        name="middle",
        grid=(1,),
        in_specs=[pl.BlockSpec(memory_space=pltpu.SMEM), full(128, D)]
        + [full(16, D)] * 8
        + [level_block(1), full(3, D), bridge_block(1), full(8, D), full(1024, 256), full(8, 128)],
        out_specs=[full(128, D), full(8, D), full(8, D)],
        out_shape=[
            jax.ShapeDtypeStruct((128, D), F32),
            jax.ShapeDtypeStruct((8, D), F32),
            jax.ShapeDtypeStruct((8, D), BF),
        ],
        compiler_params=pltpu.CompilerParams(vmem_limit_bytes=24 << 20),
        cost_estimate=pl.CostEstimate(flops=2 * 12 * 128 * D * D, bytes_accessed=5 << 20, transcendentals=1 << 20),
    )(inner, mz, *rim, pw, pb, bw, coarse, gather, mean)


def coarse_kernel(inner_ref, cz_ref, *refs):
    rim_refs = refs[:8]
    w_ref, c_ref, b2_ref, b3_ref, mo_ref, gather_ref, lift_ref, spread_out = refs[8:]
    cz = cz_ref[...]
    own = cz.astype(BF)
    recv = 0.5 * (mm(own, w_ref[0, 0]) + c_ref[2:3, :])
    pieces = [cz] + [ref[...].astype(F32) for ref in rim_refs] + [jnp.zeros((56, D), F32)]
    send = (0.5 * mm(jnp.concatenate(pieces, axis=0).astype(BF), w_ref[0, 1])).astype(BF)
    near = mm(gather_ref[...], send)
    hidden = gate(near.reshape(8, 8, D) + recv[None]).astype(BF).reshape(64, D)
    msg = gate(0.5 * mm(hidden, w_ref[0, 2])).reshape(8, 8, D)
    lat = (lax.broadcasted_iota(jnp.int32, (8, D), 0) // 2) % 2
    up = jnp.where(lat == 0, inner_ref[0], 1.0)
    down = jnp.where(lat == 1, inner_ref[1], 1.0)
    total = up * (msg[0] + msg[1] + msg[2]) + (msg[3] + msg[4]) + down * (msg[5] + msg[6] + msg[7])
    avg = (0.125 * total).astype(BF)
    co = cz + mm(avg, w_ref[0, 3])
    lifted = gate(0.5 * mm(co.astype(BF), b2_ref[0]))
    high = lifted.astype(BF).astype(F32)
    both = jnp.concatenate([high, lifted - high], axis=0).astype(BF)
    two = mo_ref[...] + mm(lift_ref[...], both)
    spread_out[...] = gate(0.5 * mm(two.astype(BF), b3_ref[0])).reshape(2, 8, 8, D)


def coarsest(inner, cz, rim, pw, pb, bw, mo, gather, lift):
    return pl.pallas_call(
        coarse_kernel,
        name="coarsest",
        grid=(1,),
        in_specs=[pl.BlockSpec(memory_space=pltpu.SMEM), full(8, D)]
        + [full(8, D)] * 8
        + [level_block(2), full(3, D), bridge_block(2), bridge_block(3), full(128, D), full(64, 128), full(128, 16)],
        out_specs=full(2, 8, 8, D),
        out_shape=jax.ShapeDtypeStruct((2, 8, 8, D), F32),
        compiler_params=pltpu.CompilerParams(vmem_limit_bytes=24 << 20),
        cost_estimate=pl.CostEstimate(flops=2 * 2 * 128 * D * D, bytes_accessed=4 << 20, transcendentals=1 << 18),
    )(inner, cz, *rim, pw, pb, bw, bw, mo, gather, lift)


FRB = 8


def finish_kernel(s_ref, avg_ref, w_ref, spread_ref, out_ref):
    one = mm(avg_ref[0].reshape(FRB * 32, D), w_ref[0, 0]).reshape(FRB, 32, D)
    first = lax.broadcasted_iota(jnp.int32, (8, D), 0) < 4
    for g in range(FRB // 4):
        parts = []
        for t in range(4):
            low = jnp.broadcast_to(spread_ref[0, g, 2 * t:2 * t + 1, :], (8, D))
            high = jnp.broadcast_to(spread_ref[0, g, 2 * t + 1:2 * t + 2, :], (8, D))
            parts.append(jnp.where(first, low, high))
        wide = jnp.concatenate(parts, axis=0)
        for i in range(4 * g, 4 * g + 4):
            out_ref[0, i] = s_ref[0, i] + one[i] + wide


def finish(fine, avg, pw, spread):
    block = pl.BlockSpec((1, FRB, 32, D), lambda b, i: (b, i, 0, 0))
    return pl.pallas_call(
        finish_kernel,
        name="finish",
        grid=(2, 32 // FRB),
        in_specs=[
            block,
            block,
            pl.BlockSpec((1, 1, D, D), lambda b, i: (0, 3, 0, 0)),
            pl.BlockSpec((1, FRB // 4, 8, D), lambda b, i: (b, i, 0, 0)),
        ],
        out_specs=block,
        out_shape=jax.ShapeDtypeStruct((2, 32, 32, D), F32),
        compiler_params=pltpu.CompilerParams(vmem_limit_bytes=24 << 20),
        cost_estimate=pl.CostEstimate(flops=2 * 2048 * D * D, bytes_accessed=10 << 20, transcendentals=0),
    )(fine, avg, pw, spread)


def place_middle():
    pick = np.zeros((128, 128), np.float32)
    for d, (p, q) in enumerate(OFFS):
        for b in range(2):
            rows = [0] if p < 0 else [7] if p > 0 else range(8)
            cols = [0] if q < 0 else [7] if q > 0 else range(8)
            for n, (i, j) in enumerate((i, j) for i in rows for j in cols):
                pick[16 * d + 8 * b + n, 64 * b + 8 * i + j] = 1
    gather = np.zeros((1024, 256), np.float32)
    for k, (p, q) in enumerate(OFFS):
        for b in range(2):
            for i in range(8):
                for j in range(8):
                    y, x = i + p, j + q
                    dy = (y > 7) - (y < 0)
                    dx = (x > 7) - (x < 0)
                    if (dy, dx) == (0, 0):
                        source = 64 * b + 8 * y + x
                    else:
                        n = 0 if dy and dx else x if dy else y
                        source = 128 + 16 * OFFS.index((dy, dx)) + 8 * b + n
                    gather[128 * k + 64 * b + 8 * i + j, source] = 1
    mean = np.zeros((8, 128), np.float32)
    for b in range(2):
        for i in range(8):
            for j in range(8):
                mean[4 * b + 2 * (i // 4) + j // 4, 64 * b + 8 * i + j] = 1 / 16
    return pick, gather, mean


def place_coarse():
    gather = np.zeros((64, 128), np.float32)
    for k, (p, q) in enumerate(OFFS):
        for b in range(2):
            for i in range(2):
                for j in range(2):
                    y, x = i + p, j + q
                    dy = (y > 1) - (y < 0)
                    dx = (x > 1) - (x < 0)
                    base = 0 if (dy, dx) == (0, 0) else 8 + 8 * OFFS.index((dy, dx))
                    gather[8 * k + 4 * b + 2 * i + j, base + 4 * b + 2 * (y % 2) + x % 2] = 1
    lift = np.zeros((128, 16), np.float32)
    for b in range(2):
        for i in range(8):
            for j in range(8):
                source = 4 * b + 2 * (i // 4) + j // 4
                lift[64 * b + 8 * i + j, source] = 1
                lift[64 * b + 8 * i + j, 8 + source] = 1
    return gather, lift


def exchange(pieces):
    rows, cols = lax.axis_size("lat"), lax.axis_size("lon")
    out = []
    for d, (p, q) in enumerate(OFFS):
        perm = []
        for y in range(rows):
            for x in range(cols):
                source = y + p
                if 0 <= source < rows:
                    perm.append((source * cols + (x + q) % cols, y * cols + x))
        out.append(lax.ppermute(pieces[7 - d], ("lat", "lon"), perm))
    return out


def local(fine, mid, coarse, flags, pw, bw, pb):
    edge_of = {-1: slice(0, 1), 1: slice(-1, None), 0: slice(None)}
    pieces = []
    for p, q in OFFS:
        part = fine[:, edge_of[p], edge_of[q], :].astype(BF)
        pieces.append(part.reshape(2, -1, D))
    rim = exchange(pieces)
    lat = lax.axis_index("lat")
    rows = lax.axis_size("lat")
    inner = jnp.stack([lat > 0, lat < rows - 1]).astype(F32)
    index = jnp.arange(32)
    step = jnp.asarray([p for p, q in OFFS])[:, None]
    where = lat * 32 + index[None, :] + step
    live = flags.astype(BF) * ((where >= 0) & (where < rows * 32)).astype(BF)[:, :, None]
    mask = jnp.broadcast_to(live[..., None], (8, 32, 32, 128))
    pick, gather, mean = place_middle()
    gather_c, lift = place_coarse()
    r, t, ps = prep(fine, pw, pb)
    ul, up, ur, left, right, dl, down, dr = rim
    avg, mz, *send = edge(r, t, (up, down, left, right, ul, ur, dl, dr), mask, pw, bw, ps, mid, jnp.asarray(pick, BF))
    rim = exchange(send)
    mo, cz, czb = middle(inner, mz, rim, pw, pb, bw, coarse.reshape(8, D), jnp.asarray(gather, BF), jnp.asarray(mean, F32))
    rim = exchange([czb] * 8)
    spread = coarsest(inner, cz, rim, pw, pb, bw, mo, jnp.asarray(gather_c, BF), jnp.asarray(lift, BF))
    return finish(fine, avg, pw, spread), avg


def solution(mesh):
    node = P(None, "lat", "lon", None)
    return jax.shard_map(
        local,
        mesh=mesh,
        in_specs=(node, node, node, P(None, "lat", "lon"), P(), P(), P()),
        out_specs=(node, node),
        check_vma=False,
    )
```

```python
import functools
import jax
import jax.numpy as jnp
import numpy as np
from jax import lax
from jax.experimental import pallas as pl
from jax.experimental.pallas import tpu as pltpu
from jax.sharding import PartitionSpec as P

D = 512
BF = jnp.bfloat16
F32 = jnp.float32
OFFS = ((-1, -1), (-1, 0), (-1, 1), (0, -1), (0, 1), (1, -1), (1, 0), (1, 1))
PRB = 8
RB = 8


def mm(a, b):
    return jnp.dot(a, b, preferred_element_type=F32)


def gate(half):
    return half + half * jnp.tanh(half)


def pool_rows(x, g, tmp):
    tall = (x[4 * g] + x[4 * g + 1]) + (x[4 * g + 2] + x[4 * g + 3])
    parts = []
    for lane in range(4):
        tmp[g, lane] = tall[:, lane * 128:(lane + 1) * 128]
        part = tmp[g, lane, pl.ds(0, 8, stride=4), :]
        for t in range(1, 4):
            part = part + tmp[g, lane, pl.ds(t, 8, stride=4), :]
        parts.append(part)
    return jnp.concatenate(parts, axis=1)


def rims_kernel(top_ref, bottom_ref, west_ref, east_ref, top_out, bottom_out, west_out, east_out):
    top_out[...] = top_ref[...].reshape(2, 32, D).astype(BF)
    bottom_out[...] = bottom_ref[...].reshape(2, 32, D).astype(BF)
    for b in range(2):
        west_out[b] = west_ref[b, :, 0, :].astype(BF)
        east_out[b] = east_ref[b, :, 7, :].astype(BF)


def rims(fine):
    out = pl.BlockSpec((2, 32, D), lambda i: (0, 0, 0))
    return pl.pallas_call(
        rims_kernel,
        name="rims",
        grid=(1,),
        in_specs=[
            pl.BlockSpec((2, 1, 32, D), lambda i: (0, 0, 0, 0)),
            pl.BlockSpec((2, 1, 32, D), lambda i: (0, 31, 0, 0)),
            pl.BlockSpec((2, 32, 8, D), lambda i: (0, 0, 0, 0)),
            pl.BlockSpec((2, 32, 8, D), lambda i: (0, 0, 3, 0)),
        ],
        out_specs=[out] * 4,
        out_shape=[jax.ShapeDtypeStruct((2, 32, D), BF)] * 4,
        compiler_params=pltpu.CompilerParams(vmem_limit_bytes=24 << 20),
        cost_estimate=pl.CostEstimate(flops=1 << 20, bytes_accessed=3 << 20, transcendentals=0),
    )(fine, fine, fine, fine)


def prep_kernel(s_ref, w_ref, c_ref, r_out, t_out, ps_out, tmp):
    x = s_ref[0]
    op = x.reshape(PRB * 32, D).astype(BF)
    r = mm(op, w_ref[0, 0])
    r_out[0] = (0.5 * (r + c_ref[0:1, :])).astype(BF).reshape(PRB, 32, D)
    t_out[0] = (0.5 * mm(op, w_ref[0, 1])).astype(BF).reshape(PRB, 32, D)
    for g in range(PRB // 4):
        ps_out[0, g] = pool_rows(x, g, tmp)


def prep(fine, pw, pb):
    return pl.pallas_call(
        prep_kernel,
        name="prep",
        grid=(2, 32 // PRB),
        in_specs=[
            pl.BlockSpec((1, PRB, 32, D), lambda b, i: (b, i, 0, 0)),
            pl.BlockSpec((1, 2, D, D), lambda b, i: (0, 0, 0, 0)),
            pl.BlockSpec((3, D), lambda b, i: (0, 0)),
        ],
        out_specs=[
            pl.BlockSpec((1, PRB, 32, D), lambda b, i: (b, i, 0, 0)),
            pl.BlockSpec((1, PRB, 32, D), lambda b, i: (b, i, 0, 0)),
            pl.BlockSpec((1, PRB // 4, 8, D), lambda b, i: (b, i, 0, 0)),
        ],
        out_shape=[
            jax.ShapeDtypeStruct((2, 32, 32, D), BF),
            jax.ShapeDtypeStruct((2, 32, 32, D), BF),
            jax.ShapeDtypeStruct((2, 8, 8, D), F32),
        ],
        scratch_shapes=[pltpu.VMEM((8, 4, 32, 128), F32)],
        compiler_params=pltpu.CompilerParams(vmem_limit_bytes=32 << 20),
        cost_estimate=pl.CostEstimate(flops=2 * 2 * 2048 * D * D, bytes_accessed=10 << 20, transcendentals=0),
    )(fine, pw, pb)


def edge_kernel(r_ref, t_ref, up_ref, down_ref, left_ref, right_ref,
                mask_ref, w_ref, b0_ref, ps_ref, mid_ref, pick_ref,
                avg_out, mz_out, *rest):
    rim_outs, (sh, hs, tmp, pa) = rest[:4], rest[4:]
    b = pl.program_id(0)
    blk = pl.program_id(1)

    @pl.when(blk == 0)
    def _():
        for n, ref in enumerate((up_ref, down_ref, left_ref, right_ref)):
            hs[n, 0:ref.shape[1], :] = (0.5 * mm(ref[0], w_ref[0, 1])).astype(BF).astype(F32)
        rows = lax.broadcasted_iota(jnp.int32, (32, D), 0)

        def put(i, x, left, right):
            sh[1, i] = x.astype(BF)
            sh[0, i] = jnp.where(rows == 0, jnp.broadcast_to(left, (32, D)), pltpu.roll(x, 1, 0)).astype(BF)
            sh[2, i] = jnp.where(rows == 31, jnp.broadcast_to(right, (32, D)), pltpu.roll(x, 31, 0)).astype(BF)

        put(0, hs[0, 0:32, :], hs[2, 32:33, :], hs[3, 32:33, :])
        put(33, hs[1, 0:32, :], hs[2, 33:34, :], hs[3, 33:34, :])

        @pl.loop(0, 32)
        def _(i):
            put(i + 1, t_ref[0, i].astype(F32), hs[2, pl.ds(i, 1), :], hs[3, pl.ds(i, 1), :])

    row0 = blk * RB
    rv = r_ref[0].reshape(RB * 32, D)
    acc = None
    for k, (p, q) in enumerate(OFFS):
        sv = sh[q + 1, pl.ds(row0 + 1 + p, RB)].reshape(RB * 32, D)
        x = rv + sv
        m = mask_ref[k].reshape(RB * 32, 128)
        h = gate(x) * jnp.concatenate([m] * 4, axis=1)
        g = 0.5 * mm(h, w_ref[0, 2])
        msg = gate(g)
        acc = msg if acc is None else acc + msg
    avg = (acc * 0.125).astype(BF)
    av = avg.reshape(RB, 32, D)
    avg_out[0] = av
    af = av.astype(F32)
    for g in range(RB // 4):
        pa[b, blk * (RB // 4) + g] = pool_rows(af, g, tmp)

    @pl.when((b == 1) & (blk == 32 // RB - 1))
    def _():
        mean_avg = (pa[...].reshape(128, D) * 0.0625).astype(BF)
        pooled = (ps_ref[...].reshape(128, D) * 0.0625 + mm(mean_avg, w_ref[0, 3])).astype(BF)
        mz = mid_ref[...].reshape(128, D) + gate(0.5 * mm(pooled, b0_ref[0]))
        mz_out[...] = mz
        rims = mm(pick_ref[...], mz.astype(BF)).astype(BF)
        for d in range(4):
            rim_outs[d][...] = rims[16 * d:16 * d + 16]


def edge(r, t, rim, mask, pw, bw, ps, mid, pick):
    whole = lambda *shape: pl.BlockSpec(shape, lambda b, i: (0,) * len(shape))
    return pl.pallas_call(
        edge_kernel,
        name="edge",
        grid=(2, 32 // RB),
        in_specs=[
            pl.BlockSpec((1, RB, 32, D), lambda b, i: (b, i, 0, 0)),
            pl.BlockSpec((1, 32, 32, D), lambda b, i: (b, 0, 0, 0)),
        ]
        + [pl.BlockSpec((1, 32, D), lambda b, i: (b, 0, 0))] * 2
        + [pl.BlockSpec((1, 34, D), lambda b, i: (b, 0, 0))] * 2
        + [
            pl.BlockSpec((8, RB, 32, 128), lambda b, i: (0, i, 0, 0)),
            whole(1, 4, D, D),
            whole(1, D, D),
            whole(2, 8, 8, D),
            whole(2, 8, 8, D),
            whole(64, 128),
        ],
        out_specs=[
            pl.BlockSpec((1, RB, 32, D), lambda b, i: (b, i, 0, 0)),
            whole(128, D),
        ]
        + [whole(16, D)] * 4,
        out_shape=[
            jax.ShapeDtypeStruct((2, 32, 32, D), BF),
            jax.ShapeDtypeStruct((128, D), F32),
        ]
        + [jax.ShapeDtypeStruct((16, D), BF)] * 4,
        scratch_shapes=[
            pltpu.VMEM((3, 34, 32, D), BF),
            pltpu.VMEM((4, 40, D), F32),
            pltpu.VMEM((8, 4, 32, 128), F32),
            pltpu.VMEM((2, 8, 8, D), F32),
        ],
        compiler_params=pltpu.CompilerParams(vmem_limit_bytes=48 << 20),
        cost_estimate=pl.CostEstimate(flops=2 * 8 * 2048 * D * D, bytes_accessed=16 << 20, transcendentals=16 << 20),
    )(r, t, *rim, mask, pw, bw, ps, mid, pick)


def middle_kernel(inner_ref, mz_ref, *refs):
    rim_refs = refs[:4]
    w_ref, c_ref, b1_ref, coarse_ref, gather_ref, mean_ref, mo_out, cz_out, czb_out = refs[4:]
    mz = mz_ref[...]
    own = mz.astype(BF)
    recv = 0.5 * (mm(own, w_ref[0, 0]) + c_ref[1:2, :])
    states = jnp.concatenate([own] + [ref[...] for ref in rim_refs], axis=0)
    send = (0.5 * mm(states, w_ref[0, 1])).astype(BF)
    near = mm(gather_ref[...], send)
    hidden = gate(near.reshape(8, 128, D) + recv[None]).astype(BF).reshape(1024, D)
    msg = gate(0.5 * mm(hidden, w_ref[0, 2])).reshape(8, 128, D)
    lat = (lax.broadcasted_iota(jnp.int32, (128, D), 0) // 8) % 8
    up = jnp.where(lat == 0, inner_ref[0], 1.0)
    down = jnp.where(lat == 7, inner_ref[1], 1.0)
    total = up * (msg[0] + msg[1] + msg[2]) + (msg[3] + msg[4]) + down * (msg[5] + msg[6] + msg[7])
    avg = (0.125 * total).astype(BF)
    mo = mz + mm(avg, w_ref[0, 3])
    mo_out[...] = mo
    pooled = jnp.dot(mean_ref[...], mo, preferred_element_type=F32, precision=lax.Precision.HIGHEST)
    cz = coarse_ref[...] + gate(0.5 * mm(pooled.astype(BF), b1_ref[0]))
    cz_out[...] = cz
    czb_out[...] = cz.astype(BF)


VM = pl.BlockSpec(memory_space=pltpu.VMEM)


def level_block(level):
    return pl.BlockSpec((1, 4, D, D), lambda i: (level, 0, 0, 0))


def bridge_block(index):
    return pl.BlockSpec((1, D, D), lambda i: (index, 0, 0))


def full(*shape):
    return pl.BlockSpec(shape, lambda i: (0,) * len(shape))


def middle(inner, mz, rim, pw, pb, bw, coarse, gather, mean):
    return pl.pallas_call(
        middle_kernel,
        name="middle",
        grid=(1,),
        in_specs=[pl.BlockSpec(memory_space=pltpu.SMEM), full(128, D)]
        + [full(16, D)] * 2
        + [full(48, D)] * 2
        + [level_block(1), full(3, D), bridge_block(1), full(8, D), full(1024, 256), full(8, 128)],
        out_specs=[full(128, D), full(8, D), full(8, D)],
        out_shape=[
            jax.ShapeDtypeStruct((128, D), F32),
            jax.ShapeDtypeStruct((8, D), F32),
            jax.ShapeDtypeStruct((8, D), BF),
        ],
        compiler_params=pltpu.CompilerParams(vmem_limit_bytes=24 << 20),
        cost_estimate=pl.CostEstimate(flops=2 * 12 * 128 * D * D, bytes_accessed=5 << 20, transcendentals=1 << 20),
    )(inner, mz, *rim, pw, pb, bw, coarse, gather, mean)


def coarse_kernel(inner_ref, cz_ref, *refs):
    rim_refs = refs[:4]
    w_ref, c_ref, b2_ref, b3_ref, mo_ref, gather_ref, lift_ref, spread_out = refs[4:]
    cz = cz_ref[...]
    own = cz.astype(BF)
    recv = 0.5 * (mm(own, w_ref[0, 0]) + c_ref[2:3, :])
    pieces = [cz] + [ref[...].astype(F32) for ref in rim_refs] + [jnp.zeros((56, D), F32)]
    send = (0.5 * mm(jnp.concatenate(pieces, axis=0).astype(BF), w_ref[0, 1])).astype(BF)
    near = mm(gather_ref[...], send)
    hidden = gate(near.reshape(8, 8, D) + recv[None]).astype(BF).reshape(64, D)
    msg = gate(0.5 * mm(hidden, w_ref[0, 2])).reshape(8, 8, D)
    lat = (lax.broadcasted_iota(jnp.int32, (8, D), 0) // 2) % 2
    up = jnp.where(lat == 0, inner_ref[0], 1.0)
    down = jnp.where(lat == 1, inner_ref[1], 1.0)
    total = up * (msg[0] + msg[1] + msg[2]) + (msg[3] + msg[4]) + down * (msg[5] + msg[6] + msg[7])
    avg = (0.125 * total).astype(BF)
    co = cz + mm(avg, w_ref[0, 3])
    lifted = gate(0.5 * mm(co.astype(BF), b2_ref[0]))
    high = lifted.astype(BF).astype(F32)
    both = jnp.concatenate([high, lifted - high], axis=0).astype(BF)
    two = mo_ref[...] + mm(lift_ref[...], both)
    spread_out[...] = gate(0.5 * mm(two.astype(BF), b3_ref[0])).reshape(2, 8, 8, D)


def coarsest(inner, cz, rim, pw, pb, bw, mo, gather, lift):
    return pl.pallas_call(
        coarse_kernel,
        name="coarsest",
        grid=(1,),
        in_specs=[pl.BlockSpec(memory_space=pltpu.SMEM), full(8, D)]
        + [full(8, D)] * 2
        + [full(24, D)] * 2
        + [level_block(2), full(3, D), bridge_block(2), bridge_block(3), full(128, D), full(64, 128), full(128, 16)],
        out_specs=full(2, 8, 8, D),
        out_shape=jax.ShapeDtypeStruct((2, 8, 8, D), F32),
        compiler_params=pltpu.CompilerParams(vmem_limit_bytes=24 << 20),
        cost_estimate=pl.CostEstimate(flops=2 * 2 * 128 * D * D, bytes_accessed=4 << 20, transcendentals=1 << 18),
    )(inner, cz, *rim, pw, pb, bw, bw, mo, gather, lift)


FRB = 8


def finish_kernel(s_ref, avg_ref, w_ref, spread_ref, out_ref):
    one = mm(avg_ref[0].reshape(FRB * 32, D), w_ref[0, 0]).reshape(FRB, 32, D)
    first = lax.broadcasted_iota(jnp.int32, (8, D), 0) < 4
    for g in range(FRB // 4):
        parts = []
        for t in range(4):
            low = jnp.broadcast_to(spread_ref[0, g, 2 * t:2 * t + 1, :], (8, D))
            high = jnp.broadcast_to(spread_ref[0, g, 2 * t + 1:2 * t + 2, :], (8, D))
            parts.append(jnp.where(first, low, high))
        wide = jnp.concatenate(parts, axis=0)
        for i in range(4 * g, 4 * g + 4):
            out_ref[0, i] = s_ref[0, i] + one[i] + wide


def finish(fine, avg, pw, spread):
    block = pl.BlockSpec((1, FRB, 32, D), lambda b, i: (b, i, 0, 0))
    return pl.pallas_call(
        finish_kernel,
        name="finish",
        grid=(2, 32 // FRB),
        in_specs=[
            block,
            block,
            pl.BlockSpec((1, 1, D, D), lambda b, i: (0, 3, 0, 0)),
            pl.BlockSpec((1, FRB // 4, 8, D), lambda b, i: (b, i, 0, 0)),
        ],
        out_specs=block,
        out_shape=jax.ShapeDtypeStruct((2, 32, 32, D), F32),
        compiler_params=pltpu.CompilerParams(vmem_limit_bytes=24 << 20),
        cost_estimate=pl.CostEstimate(flops=2 * 2048 * D * D, bytes_accessed=10 << 20, transcendentals=0),
    )(fine, avg, pw, spread)


def place_middle():
    pick = np.zeros((64, 128), np.float32)
    for b in range(2):
        for n in range(8):
            for d, (i, j) in enumerate(((0, n), (7, n), (n, 0), (n, 7))):
                pick[16 * d + 8 * b + n, 64 * b + 8 * i + j] = 1
    gather = np.zeros((1024, 256), np.float32)
    for k, (p, q) in enumerate(OFFS):
        for b in range(2):
            for i in range(8):
                for j in range(8):
                    y, x = i + p, j + q
                    if 0 <= x < 8:
                        n = 128 + 8 * b + x if y < 0 else 144 + 8 * b + x if y > 7 else 64 * b + 8 * y + x
                    else:
                        base = 160 + 8 * b if x < 0 else 208 + 8 * b
                        n = base + 16 + x % 8 if y < 0 else base + 32 + x % 8 if y > 7 else base + y
                    gather[128 * k + 64 * b + 8 * i + j, n] = 1
    mean = np.zeros((8, 128), np.float32)
    for b in range(2):
        for i in range(8):
            for j in range(8):
                mean[4 * b + 2 * (i // 4) + j // 4, 64 * b + 8 * i + j] = 1 / 16
    return pick, gather, mean


def place_coarse():
    gather = np.zeros((64, 128), np.float32)
    for k, (p, q) in enumerate(OFFS):
        for b in range(2):
            for i in range(2):
                for j in range(2):
                    y, x = i + p, j + q
                    base = (24 if x < 0 else 48 if x > 1 else 0) + (8 if y < 0 else 16 if y > 1 else 0)
                    gather[8 * k + 4 * b + 2 * i + j, base + 4 * b + 2 * (y % 2) + x % 2] = 1
    lift = np.zeros((128, 16), np.float32)
    for b in range(2):
        for i in range(8):
            for j in range(8):
                source = 4 * b + 2 * (i // 4) + j // 4
                lift[64 * b + 8 * i + j, source] = 1
                lift[64 * b + 8 * i + j, 8 + source] = 1
    return gather, lift


def trade(low_side, high_side, axis):
    count = lax.axis_size(axis)
    forward = [(i, (i + 1) % count) for i in range(count)]
    backward = [(i, (i - 1) % count) for i in range(count)]
    return lax.ppermute(high_side, axis, forward), lax.ppermute(low_side, axis, backward)


def local(fine, mid, coarse, flags, pw, bw, pb):
    fine, pw, bw = (pltpu.with_memory_space_constraint(a, pltpu.HBM) for a in (fine, pw, bw))
    top, bottom, west, east = rims(fine)
    up, down = trade(top, bottom, "lat")
    left, right = trade(
        jnp.concatenate([west, up[:, :1], down[:, :1]], axis=1),
        jnp.concatenate([east, up[:, 31:], down[:, 31:]], axis=1),
        "lon",
    )
    lat = lax.axis_index("lat")
    rows = lax.axis_size("lat")
    inner = jnp.stack([lat > 0, lat < rows - 1]).astype(F32)
    index = jnp.arange(32)
    step = jnp.asarray([p for p, q in OFFS])[:, None]
    where = lat * 32 + index[None, :] + step
    live = flags.astype(BF) * ((where >= 0) & (where < rows * 32)).astype(BF)[:, :, None]
    mask = jnp.broadcast_to(live[..., None], (8, 32, 32, 128))
    pick, gather, mean = place_middle()
    gather_c, lift = place_coarse()
    r, t, ps = prep(fine, pw, pb)
    avg, mz, top, bottom, west, east = edge(r, t, (up, down, left, right), mask, pw, bw, ps, mid, jnp.asarray(pick, BF))
    up, down = trade(top, bottom, "lat")
    left, right = trade(jnp.concatenate([west, up, down]), jnp.concatenate([east, up, down]), "lon")
    mo, cz, czb = middle(
        inner, mz, (up, down, left, right), pw, pb, bw, coarse.reshape(8, D), jnp.asarray(gather, BF), jnp.asarray(mean, F32)
    )
    up, down = trade(czb, czb, "lat")
    column = jnp.concatenate([czb, up, down])
    left, right = trade(column, column, "lon")
    spread = coarsest(
        inner, cz, (up, down, left, right), pw, pb, bw, mo, jnp.asarray(gather_c, BF), jnp.asarray(lift, BF)
    )
    return finish(fine, avg, pw, spread), avg


def solution(mesh):
    node = P(None, "lat", "lon", None)
    return jax.shard_map(
        local,
        mesh=mesh,
        in_specs=(node, node, node, P(None, "lat", "lon"), P(), P(), P()),
        out_specs=(node, node),
        check_vma=False,
    )
```

```python
import functools
import jax
import jax.numpy as jnp
import numpy as np
from jax import lax
from jax.experimental import pallas as pl
from jax.experimental.pallas import tpu as pltpu
from jax.sharding import PartitionSpec as P

D = 512
ANY = pl.BlockSpec(memory_space=pl.ANY)
BF = jnp.bfloat16
F32 = jnp.float32
OFFS = ((-1, -1), (-1, 0), (-1, 1), (0, -1), (0, 1), (1, -1), (1, 0), (1, 1))
PRB = 8
EDGE_VMEM = 28
RB = 8
EDGE_VMEM = 28


def mm(a, b):
    return jnp.dot(a, b, preferred_element_type=F32)


def gate(half):
    return half + half * jnp.tanh(half)


def pool_rows(x, g, tmp):
    tall = (x[4 * g] + x[4 * g + 1]) + (x[4 * g + 2] + x[4 * g + 3])
    parts = []
    for lane in range(4):
        tmp[g, lane] = tall[:, lane * 128:(lane + 1) * 128]
        part = tmp[g, lane, pl.ds(0, 8, stride=4), :]
        for t in range(1, 4):
            part = part + tmp[g, lane, pl.ds(t, 8, stride=4), :]
        parts.append(part)
    return jnp.concatenate(parts, axis=1)


def rims_kernel(top_ref, bottom_ref, west_ref, east_ref, top_out, bottom_out, west_out, east_out):
    top_out[...] = top_ref[...].reshape(2, 32, D).astype(BF)
    bottom_out[...] = bottom_ref[...].reshape(2, 32, D).astype(BF)
    for b in range(2):
        west_out[b] = west_ref[b, :, 0, :].astype(BF)
        east_out[b] = east_ref[b, :, 7, :].astype(BF)


def rims(fine):
    out = pl.BlockSpec((2, 32, D), lambda i: (0, 0, 0))
    return pl.pallas_call(
        rims_kernel,
        name="rims",
        grid=(1,),
        in_specs=[
            pl.BlockSpec((2, 1, 32, D), lambda i: (0, 0, 0, 0)),
            pl.BlockSpec((2, 1, 32, D), lambda i: (0, 31, 0, 0)),
            pl.BlockSpec((2, 32, 8, D), lambda i: (0, 0, 0, 0)),
            pl.BlockSpec((2, 32, 8, D), lambda i: (0, 0, 3, 0)),
        ],
        out_specs=[out] * 4,
        out_shape=[jax.ShapeDtypeStruct((2, 32, D), BF)] * 4,
        compiler_params=pltpu.CompilerParams(vmem_limit_bytes=24 << 20),
        cost_estimate=pl.CostEstimate(flops=1 << 20, bytes_accessed=3 << 20, transcendentals=0),
    )(fine, fine, fine, fine)


def prep_kernel(s_hbm, w_hbm, c_ref, rt_out, s_ref, w_ref, sems, w_sem):
    weights = pltpu.make_async_copy(w_hbm.at[0, 0:2], w_ref, w_sem)
    weights.start()
    copies = []
    for n in range(8):
        at = (n // 4, pl.ds(8 * (n % 4), 8))
        copies.append(pltpu.make_async_copy(s_hbm.at[at], s_ref.at[n], sems.at[n]))
        copies[-1].start()
    weights.wait()
    for n in range(8):
        copies[n].wait()
        b, i = n // 4, n % 4
        x = s_ref[n]
        op = x.reshape(256, D).astype(BF)
        rt_out[0, b, 8 * i:8 * i + 8] = (0.5 * (mm(op, w_ref[0]) + c_ref[0:1, :])).astype(BF).reshape(8, 32, D)
        rt_out[1, b, 8 * i:8 * i + 8] = (0.5 * mm(op, w_ref[1])).astype(BF).reshape(8, 32, D)


def prep(fine, pw, pb):
    full4 = lambda *shape: pl.BlockSpec(shape, lambda i: (0,) * len(shape))
    return pl.pallas_call(
        prep_kernel,
        name="prep",
        grid=(1,),
        in_specs=[ANY, ANY, full4(3, D)],
        out_specs=full4(2, 2, 32, 32, D),
        out_shape=pltpu.VMEM((2, 2, 32, 32, D), BF),
        scratch_shapes=[
            pltpu.VMEM((8, 8, 32, D), F32),
            pltpu.VMEM((2, D, D), BF),
            pltpu.SemaphoreType.DMA((8,)),
            pltpu.SemaphoreType.DMA,
        ],
        compiler_params=pltpu.CompilerParams(vmem_limit_bytes=24 << 20),
        cost_estimate=pl.CostEstimate(flops=2 * 2 * 2048 * D * D, bytes_accessed=5 << 20, transcendentals=0),
    )(fine, pw, pb)


def edge_kernel(rt_ref, up_ref, down_ref, left_ref, right_ref,
                live_ref, w_ref, b0_ref, mid_ref, pick_ref, s_ref, pw_hbm, bw_hbm,
                avg_out, one_out, mz_out, *rest):
    rim_outs, (w1_out, w2_out, b1_out, b23_out, sh, hs, tmp, pa, hid, w2_half, sems) = rest[:4], rest[4:]
    b = pl.program_id(0)
    blk = pl.program_id(1)

    ahead = [
        pltpu.make_async_copy(pw_hbm.at[1], w1_out, sems.at[0]),
        pltpu.make_async_copy(pw_hbm.at[2], w2_out, sems.at[1]),
        pltpu.make_async_copy(bw_hbm.at[1], b1_out, sems.at[2]),
        pltpu.make_async_copy(bw_hbm.at[2:4], b23_out, sems.at[3]),
    ]

    @pl.when((b == 0) & (blk == 0))
    def _():
        for copy in ahead:
            copy.start()
        w2_half[...] = (w_ref[0, 2].astype(F32) * 0.5).astype(BF)

    @pl.when(blk == 0)
    def _():
        for n, ref in enumerate((up_ref, down_ref, left_ref, right_ref)):
            hs[n, 0:ref.shape[1], :] = (0.5 * mm(ref[0], w_ref[0, 1])).astype(BF).astype(F32)
        rows = lax.broadcasted_iota(jnp.int32, (32, D), 0)

        def put(i, x, left, right):
            sh[1, i] = x.astype(BF)
            sh[0, i] = jnp.where(rows == 0, jnp.broadcast_to(left, (32, D)), pltpu.roll(x, 1, 0)).astype(BF)
            sh[2, i] = jnp.where(rows == 31, jnp.broadcast_to(right, (32, D)), pltpu.roll(x, 31, 0)).astype(BF)

        put(0, hs[0, 0:32, :], hs[2, 32:33, :], hs[3, 32:33, :])
        put(33, hs[1, 0:32, :], hs[2, 33:34, :], hs[3, 33:34, :])

        @pl.loop(0, 32)
        def _(i):
            put(i + 1, rt_ref[1, b, i].astype(F32), hs[2, pl.ds(i, 1), :], hs[3, pl.ds(i, 1), :])

    row0 = blk * RB
    rv = rt_ref[0, b, pl.ds(row0, RB)].reshape(RB * 32, D)
    live = live_ref[...].reshape(RB * 32, 8)
    span = RB * 32
    for k, (p, q) in enumerate(OFFS):
        sv = sh[q + 1, pl.ds(row0 + 1 + p, RB)].reshape(span, D)
        m = jnp.broadcast_to(live[:, k:k + 1], (span, 128)).astype(BF)
        hid[k * span:(k + 1) * span] = gate(rv + sv) * jnp.concatenate([m] * 4, axis=1)
    msg = gate(mm(hid[...], w2_half[...])).reshape(8, span, D)
    avg = (jnp.sum(msg, axis=0) * 0.125).astype(BF)
    avg_out[0] = avg.reshape(RB, 32, D)
    one = s_ref[0] + mm(avg, w_ref[0, 3]).reshape(RB, 32, D)
    one_out[0] = one
    for g in range(RB // 4):
        pa[b, blk * (RB // 4) + g] = pool_rows(one, g, tmp)

    @pl.when((b == 1) & (blk == 32 // RB - 1))
    def _():
        pooled = (pa[...].reshape(128, D) * 0.0625).astype(BF)
        mz = mid_ref[...].reshape(128, D) + gate(0.5 * mm(pooled, b0_ref[0]))
        mz_out[...] = mz
        rims = mm(pick_ref[...], mz.astype(BF)).astype(BF)
        for d in range(4):
            rim_outs[d][...] = rims[16 * d:16 * d + 16]
        for copy in ahead:
            copy.wait()


def edge(rt, rim, mask, pw, bw, mid, pick, fine):
    whole = lambda *shape: pl.BlockSpec(shape, lambda b, i: (0,) * len(shape))
    return pl.pallas_call(
        edge_kernel,
        name="edge",
        grid=(2, 32 // RB),
        in_specs=[
            VM,
        ]
        + [pl.BlockSpec((1, 32, D), lambda b, i: (b, 0, 0))] * 2
        + [pl.BlockSpec((1, 34, D), lambda b, i: (b, 0, 0))] * 2
        + [
            pl.BlockSpec((RB, 32, 8), lambda b, i: (i, 0, 0)),
            whole(1, 4, D, D),
            whole(1, D, D),
            whole(2, 8, 8, D),
            whole(64, 128),
            pl.BlockSpec((1, RB, 32, D), lambda b, i: (b, i, 0, 0)),
            ANY,
            ANY,
        ],
        out_specs=[
            pl.BlockSpec((1, RB, 32, D), lambda b, i: (b, i, 0, 0)),
            pl.BlockSpec((1, RB, 32, D), lambda b, i: (b, i, 0, 0)),
            whole(128, D),
        ]
        + [whole(16, D)] * 4
        + [pl.BlockSpec(memory_space=pltpu.VMEM)] * 4,
        out_shape=[
            jax.ShapeDtypeStruct((2, 32, 32, D), BF),
            jax.ShapeDtypeStruct((2, 32, 32, D), F32),
            jax.ShapeDtypeStruct((128, D), F32),
        ]
        + [jax.ShapeDtypeStruct((16, D), BF)] * 4
        + [
            pltpu.VMEM((4, D, D), BF),
            pltpu.VMEM((4, D, D), BF),
            pltpu.VMEM((D, D), BF),
            pltpu.VMEM((2, D, D), BF),
        ],
        scratch_shapes=[
            pltpu.VMEM((3, 34, 32, D), BF),
            pltpu.VMEM((4, 40, D), F32),
            pltpu.VMEM((8, 4, 32, 128), F32),
            pltpu.VMEM((2, 8, 8, D), F32),
            pltpu.VMEM((8 * RB * 32, D), BF),
            pltpu.VMEM((D, D), BF),
            pltpu.SemaphoreType.DMA((4,)),
        ],
        compiler_params=pltpu.CompilerParams(vmem_limit_bytes=EDGE_VMEM << 20),
        cost_estimate=pl.CostEstimate(flops=2 * 8 * 2048 * D * D, bytes_accessed=16 << 20, transcendentals=16 << 20),
    )(rt, *rim, mask, pw, bw, mid, pick, fine, pw, bw)


def live_sides(first, last):
    at, count = lax.axis_index("lat"), lax.axis_size("lat")
    up = jnp.where(at > 0, 1.0, 0.0).astype(F32)
    down = jnp.where(at < count - 1, 1.0, 0.0).astype(F32)
    return jnp.where(first, up, 1.0), jnp.where(last, down, 1.0)


def middle_kernel(mz_ref, *refs):
    rim_refs = refs[:4]
    w_ref, c_ref, b1_ref, coarse_ref, gather_ref, mean_ref, mo_out, cz_out, czb_out, flat = refs[4:]
    for n in range(4):
        flat[2 * n:2 * n + 2, :] = coarse_ref[n // 2, n % 2]
    mz = mz_ref[...]
    own = mz.astype(BF)
    recv = 0.5 * (mm(own, w_ref[0]) + c_ref[1:2, :])
    states = jnp.concatenate([own] + [ref[...] for ref in rim_refs], axis=0)
    send = (0.5 * mm(states, w_ref[1])).astype(BF)
    near = mm(gather_ref[...], send)
    hidden = gate(near.reshape(8, 128, D) + recv[None]).astype(BF).reshape(1024, D)
    msg = gate(0.5 * mm(hidden, w_ref[2])).reshape(8, 128, D)
    lat = (lax.broadcasted_iota(jnp.int32, (128, D), 0) // 8) % 8
    up, down = live_sides(lat == 0, lat == 7)
    total = up * (msg[0] + msg[1] + msg[2]) + (msg[3] + msg[4]) + down * (msg[5] + msg[6] + msg[7])
    avg = (0.125 * total).astype(BF)
    mo = mz + mm(avg, w_ref[3])
    mo_out[...] = mo
    pooled = jnp.dot(mean_ref[...], mo, preferred_element_type=F32, precision=lax.Precision.HIGHEST)
    cz = flat[...] + gate(0.5 * mm(pooled.astype(BF), b1_ref[...]))
    cz_out[...] = cz
    czb_out[...] = cz.astype(BF)


VM = pl.BlockSpec(memory_space=pltpu.VMEM)


def full(*shape):
    return pl.BlockSpec(shape, lambda i: (0,) * len(shape))


def middle(mz, rim, pw, pb, bw, coarse, gather, mean):
    return pl.pallas_call(
        middle_kernel,
        name="middle",
        grid=(1,),
        in_specs=[full(128, D)]
        + [full(16, D)] * 2
        + [full(48, D)] * 2
        + [VM, full(3, D), VM, full(2, 2, 2, D), full(1024, 256), full(8, 128)],
        out_specs=[full(128, D), full(8, D), full(8, D)],
        out_shape=[
            jax.ShapeDtypeStruct((128, D), F32),
            jax.ShapeDtypeStruct((8, D), F32),
            jax.ShapeDtypeStruct((8, D), BF),
        ],
        scratch_shapes=[pltpu.VMEM((8, D), F32)],
        compiler_params=pltpu.CompilerParams(vmem_limit_bytes=24 << 20),
        cost_estimate=pl.CostEstimate(flops=2 * 12 * 128 * D * D, bytes_accessed=5 << 20, transcendentals=1 << 20),
    )(mz, *rim, pw, pb, bw, coarse, gather, mean)


def coarse_kernel(cz_ref, *refs):
    rim_refs = refs[:4]
    w_ref, c_ref, b23_ref, mo_ref, gather_ref, lift_ref, one_hbm, out_hbm, buf, sems = refs[4:]
    loads = []
    for n in range(8):
        at = (n // 4, pl.ds(8 * (n % 4), 8))
        loads.append(pltpu.make_async_copy(one_hbm.at[at], buf.at[n], sems.at[n, 0]))
        loads[-1].start()
    cz = cz_ref[...]
    own = cz.astype(BF)
    recv = 0.5 * (mm(own, w_ref[0]) + c_ref[2:3, :])
    pieces = [cz] + [ref[...].astype(F32) for ref in rim_refs] + [jnp.zeros((56, D), F32)]
    send = (0.5 * mm(jnp.concatenate(pieces, axis=0).astype(BF), w_ref[1])).astype(BF)
    near = mm(gather_ref[...], send)
    hidden = gate(near.reshape(8, 8, D) + recv[None]).astype(BF).reshape(64, D)
    msg = gate(0.5 * mm(hidden, w_ref[2])).reshape(8, 8, D)
    lat = (lax.broadcasted_iota(jnp.int32, (8, D), 0) // 2) % 2
    up, down = live_sides(lat == 0, lat == 1)
    total = up * (msg[0] + msg[1] + msg[2]) + (msg[3] + msg[4]) + down * (msg[5] + msg[6] + msg[7])
    avg = (0.125 * total).astype(BF)
    co = cz + mm(avg, w_ref[3])
    lifted = gate(0.5 * mm(co.astype(BF), b23_ref[0]))
    high = lifted.astype(BF).astype(F32)
    both = jnp.concatenate([high, lifted - high], axis=0).astype(BF)
    two = mo_ref[...] + mm(lift_ref[...], both)
    spread = gate(0.5 * mm(two.astype(BF), b23_ref[1])).reshape(16, 8, D)
    first = lax.broadcasted_iota(jnp.int32, (8, D), 0) < 4
    copies = []
    for n in range(8):
        loads[n].wait()
        for g in range(2):
            parts = []
            for t in range(4):
                low = jnp.broadcast_to(spread[2 * n + g, 2 * t:2 * t + 1, :], (8, D))
                high = jnp.broadcast_to(spread[2 * n + g, 2 * t + 1:2 * t + 2, :], (8, D))
                parts.append(jnp.where(first, low, high))
            wide = jnp.concatenate(parts, axis=0)
            for i in range(4 * g, 4 * g + 4):
                buf[n, i] = buf[n, i] + wide
        copies.append(pltpu.make_async_copy(buf.at[n], out_hbm.at[n // 4, pl.ds(8 * (n % 4), 8)], sems.at[n, 1]))
        copies[-1].start()
    for copy in copies:
        copy.wait()


def coarsest(cz, rim, pw, pb, bw, mo, gather, lift, one):
    return pl.pallas_call(
        coarse_kernel,
        name="coarsest",
        grid=(1,),
        in_specs=[full(8, D)]
        + [full(8, D)] * 2
        + [full(24, D)] * 2
        + [VM, full(3, D), VM, full(128, D), full(64, 128), full(128, 16), ANY],
        out_specs=ANY,
        out_shape=jax.ShapeDtypeStruct((2, 32, 32, D), F32),
        scratch_shapes=[pltpu.VMEM((8, 8, 32, D), F32), pltpu.SemaphoreType.DMA((8, 2))],
        compiler_params=pltpu.CompilerParams(vmem_limit_bytes=24 << 20),
        cost_estimate=pl.CostEstimate(flops=2 * 2 * 128 * D * D, bytes_accessed=4 << 20, transcendentals=1 << 18),
    )(cz, *rim, pw, pb, bw, mo, gather, lift, one)


def place_middle():
    pick = np.zeros((64, 128), np.float32)
    for b in range(2):
        for n in range(8):
            for d, (i, j) in enumerate(((0, n), (7, n), (n, 0), (n, 7))):
                pick[16 * d + 8 * b + n, 64 * b + 8 * i + j] = 1
    gather = np.zeros((1024, 256), np.float32)
    for k, (p, q) in enumerate(OFFS):
        for b in range(2):
            for i in range(8):
                for j in range(8):
                    y, x = i + p, j + q
                    if 0 <= x < 8:
                        n = 128 + 8 * b + x if y < 0 else 144 + 8 * b + x if y > 7 else 64 * b + 8 * y + x
                    else:
                        base = 160 + 8 * b if x < 0 else 208 + 8 * b
                        n = base + 16 + x % 8 if y < 0 else base + 32 + x % 8 if y > 7 else base + y
                    gather[128 * k + 64 * b + 8 * i + j, n] = 1
    mean = np.zeros((8, 128), np.float32)
    for b in range(2):
        for i in range(8):
            for j in range(8):
                mean[4 * b + 2 * (i // 4) + j // 4, 64 * b + 8 * i + j] = 1 / 16
    return pick, gather, mean


def place_coarse():
    gather = np.zeros((64, 128), np.float32)
    for k, (p, q) in enumerate(OFFS):
        for b in range(2):
            for i in range(2):
                for j in range(2):
                    y, x = i + p, j + q
                    base = (24 if x < 0 else 48 if x > 1 else 0) + (8 if y < 0 else 16 if y > 1 else 0)
                    gather[8 * k + 4 * b + 2 * i + j, base + 4 * b + 2 * (y % 2) + x % 2] = 1
    lift = np.zeros((128, 16), np.float32)
    for b in range(2):
        for i in range(8):
            for j in range(8):
                source = 4 * b + 2 * (i // 4) + j // 4
                lift[64 * b + 8 * i + j, source] = 1
                lift[64 * b + 8 * i + j, 8 + source] = 1
    return gather, lift


def trade(low_side, high_side, axis):
    count = lax.axis_size(axis)
    forward = [(i, (i + 1) % count) for i in range(count)]
    backward = [(i, (i - 1) % count) for i in range(count)]
    return lax.ppermute(high_side, axis, forward), lax.ppermute(low_side, axis, backward)


def local(fine, mid, coarse, flags, pw, bw, pb):
    fine, pw, bw = (pltpu.with_memory_space_constraint(a, pltpu.HBM) for a in (fine, pw, bw))
    top, bottom, west, east = rims(fine)
    up, down = trade(top, bottom, "lat")
    left, right = trade(
        jnp.concatenate([west, up[:, :1], down[:, :1]], axis=1),
        jnp.concatenate([east, up[:, 31:], down[:, 31:]], axis=1),
        "lon",
    )
    lat = lax.axis_index("lat")
    rows = lax.axis_size("lat")
    index = jnp.arange(32)
    step = jnp.asarray([p for p, q in OFFS])[:, None]
    where = lat * 32 + index[None, :] + step
    live = flags.astype(F32) * ((where >= 0) & (where < rows * 32)).astype(F32)[:, :, None]
    mask = jnp.transpose(live, (1, 2, 0))
    pick, gather, mean = place_middle()
    gather_c, lift = place_coarse()
    rt = prep(fine, pw, pb)
    avg, one, mz, top, bottom, west, east, w1, w2, b1, b23 = edge(
        rt, (up, down, left, right), mask, pw, bw, mid, jnp.asarray(pick, BF), fine
    )
    one = pltpu.with_memory_space_constraint(one, pltpu.HBM)
    up, down = trade(top, bottom, "lat")
    left, right = trade(jnp.concatenate([west, up, down]), jnp.concatenate([east, up, down]), "lon")
    mo, cz, czb = middle(
        mz, (up, down, left, right), w1, pb, b1, coarse, jnp.asarray(gather, BF), jnp.asarray(mean, F32)
    )
    up, down = trade(czb, czb, "lat")
    column = jnp.concatenate([czb, up, down])
    left, right = trade(column, column, "lon")
    refined = coarsest(
        cz, (up, down, left, right), w2, pb, b23, mo, jnp.asarray(gather_c, BF), jnp.asarray(lift, BF), one
    )
    return refined, avg


def solution(mesh):
    node = P(None, "lat", "lon", None)
    return jax.shard_map(
        local,
        mesh=mesh,
        in_specs=(node, node, node, P(None, "lat", "lon"), P(), P(), P()),
        out_specs=(node, node),
        check_vma=False,
    )
```

```python
import functools
import jax
import jax.numpy as jnp
import numpy as np
from jax import lax
from jax.experimental import pallas as pl
from jax.experimental.pallas import tpu as pltpu
from jax.sharding import PartitionSpec as P

D = 512
ANY = pl.BlockSpec(memory_space=pl.ANY)
BF = jnp.bfloat16
F32 = jnp.float32
OFFS = ((-1, -1), (-1, 0), (-1, 1), (0, -1), (0, 1), (1, -1), (1, 0), (1, 1))
PRB = 8
EDGE_VMEM = 28
RB = 8
EDGE_VMEM = 28


def mm(a, b):
    return jnp.dot(a, b, preferred_element_type=F32)


def gate(half):
    return half + half * jnp.tanh(half)


def pool_rows(x, g, tmp):
    tall = (x[4 * g] + x[4 * g + 1]) + (x[4 * g + 2] + x[4 * g + 3])
    parts = []
    for lane in range(4):
        tmp[g, lane] = tall[:, lane * 128:(lane + 1) * 128]
        part = tmp[g, lane, pl.ds(0, 8, stride=4), :]
        for t in range(1, 4):
            part = part + tmp[g, lane, pl.ds(t, 8, stride=4), :]
        parts.append(part)
    return jnp.concatenate(parts, axis=1)


def rows_kernel(top_ref, bottom_ref, top_out, bottom_out):
    top_out[...] = top_ref[...].reshape(2, 32, D).astype(BF)
    bottom_out[...] = bottom_ref[...].reshape(2, 32, D).astype(BF)


def columns_kernel(west_ref, east_ref, west_out, east_out):
    for b in range(2):
        west_out[b] = west_ref[b, :, 0, :].astype(BF)
        east_out[b] = east_ref[b, :, 7, :].astype(BF)


def rims(body, shape, first, last, fine):
    out = pl.BlockSpec((2, 32, D), lambda i: (0, 0, 0))
    return pl.pallas_call(
        body,
        name=body.__name__,
        grid=(1,),
        in_specs=[pl.BlockSpec(shape, lambda i: first), pl.BlockSpec(shape, lambda i: last)],
        out_specs=[out] * 2,
        out_shape=[jax.ShapeDtypeStruct((2, 32, D), BF)] * 2,
        compiler_params=pltpu.CompilerParams(vmem_limit_bytes=24 << 20),
        cost_estimate=pl.CostEstimate(flops=1 << 24, bytes_accessed=3 << 20, transcendentals=0),
    )(fine, fine)


def prep_kernel(s_hbm, w_hbm, c_ref, rt_out, s_ref, w_ref, sems, w_sem):
    weights = pltpu.make_async_copy(w_hbm.at[0, 0:2], w_ref, w_sem)
    weights.start()
    copies = []
    for n in range(4):
        at = (n // 2, pl.ds(16 * (n % 2), 16))
        copies.append(pltpu.make_async_copy(s_hbm.at[at], s_ref.at[n], sems.at[n]))
        copies[-1].start()
    weights.wait()
    for n in range(4):
        copies[n].wait()
        b, i = n // 2, n % 2
        x = s_ref[n]
        op = x.reshape(512, D).astype(BF)
        rt_out[0, b, 16 * i:16 * i + 16] = (0.5 * (mm(op, w_ref[0]) + c_ref[0:1, :])).astype(BF).reshape(16, 32, D)
        rt_out[1, b, 16 * i:16 * i + 16] = (0.5 * mm(op, w_ref[1])).astype(BF).reshape(16, 32, D)


def prep(fine, pw, pb):
    full4 = lambda *shape: pl.BlockSpec(shape, lambda i: (0,) * len(shape))
    return pl.pallas_call(
        prep_kernel,
        name="prep",
        grid=(1,),
        in_specs=[ANY, ANY, full4(3, D)],
        out_specs=full4(2, 2, 32, 32, D),
        out_shape=pltpu.VMEM((2, 2, 32, 32, D), BF),
        scratch_shapes=[
            pltpu.VMEM((4, 16, 32, D), F32),
            pltpu.VMEM((2, D, D), BF),
            pltpu.SemaphoreType.DMA((4,)),
            pltpu.SemaphoreType.DMA,
        ],
        compiler_params=pltpu.CompilerParams(vmem_limit_bytes=24 << 20),
        cost_estimate=pl.CostEstimate(flops=2 * 2 * 2048 * D * D, bytes_accessed=5 << 20, transcendentals=0),
    )(fine, pw, pb)


def edge_kernel(rt_ref, up_ref, down_ref, left_ref, right_ref,
                live_ref, w_ref, b0_ref, mid_ref, pick_ref, s_ref, pw_hbm, bw_hbm,
                avg_out, one_out, mz_out, *rest):
    rim_outs, (w1_out, w2_out, b1_out, b23_out, sh, hs, tmp, pa, hid, w2_half, sems) = rest[:4], rest[4:]
    b = pl.program_id(0)
    blk = pl.program_id(1)

    ahead = [
        pltpu.make_async_copy(pw_hbm.at[1], w1_out, sems.at[0]),
        pltpu.make_async_copy(pw_hbm.at[2], w2_out, sems.at[1]),
        pltpu.make_async_copy(bw_hbm.at[1], b1_out, sems.at[2]),
        pltpu.make_async_copy(bw_hbm.at[2:4], b23_out, sems.at[3]),
    ]

    @pl.when((b == 0) & (blk == 0))
    def _():
        for copy in ahead:
            copy.start()
        w2_half[...] = (w_ref[0, 2].astype(F32) * 0.5).astype(BF)

    @pl.when(blk == 0)
    def _():
        for n, ref in enumerate((up_ref, down_ref, left_ref, right_ref)):
            hs[n, 0:ref.shape[1], :] = (0.5 * mm(ref[0], w_ref[0, 1])).astype(BF).astype(F32)
        rows = lax.broadcasted_iota(jnp.int32, (32, D), 0)

        def put(i, x, left, right):
            sh[1, i] = x.astype(BF)
            sh[0, i] = jnp.where(rows == 0, jnp.broadcast_to(left, (32, D)), pltpu.roll(x, 1, 0)).astype(BF)
            sh[2, i] = jnp.where(rows == 31, jnp.broadcast_to(right, (32, D)), pltpu.roll(x, 31, 0)).astype(BF)

        put(0, hs[0, 0:32, :], hs[2, 32:33, :], hs[3, 32:33, :])
        put(33, hs[1, 0:32, :], hs[2, 33:34, :], hs[3, 33:34, :])

        @pl.loop(0, 32, unroll=4)
        def _(i):
            put(i + 1, rt_ref[1, b, i].astype(F32), hs[2, pl.ds(i, 1), :], hs[3, pl.ds(i, 1), :])

    row0 = blk * RB
    rv = rt_ref[0, b, pl.ds(row0, RB)].reshape(RB * 32, D)
    live = live_ref[...].reshape(RB * 32, 8)
    span = RB * 32
    for k, (p, q) in enumerate(OFFS):
        sv = sh[q + 1, pl.ds(row0 + 1 + p, RB)].reshape(span, D)
        m = jnp.broadcast_to(live[:, k:k + 1], (span, 128)).astype(BF)
        hid[k * span:(k + 1) * span] = gate(rv + sv) * jnp.concatenate([m] * 4, axis=1)
    msg = gate(mm(hid[...], w2_half[...])).reshape(8, span, D)
    avg = (jnp.sum(msg, axis=0) * 0.125).astype(BF)
    avg_out[0] = avg.reshape(RB, 32, D)
    one = s_ref[0] + mm(avg, w_ref[0, 3]).reshape(RB, 32, D)
    one_out[0] = one
    for g in range(RB // 4):
        pa[b, blk * (RB // 4) + g] = pool_rows(one, g, tmp)

    @pl.when((b == 1) & (blk == 32 // RB - 1))
    def _():
        pooled = (pa[...].reshape(128, D) * 0.0625).astype(BF)
        mz = mid_ref[...].reshape(128, D) + gate(0.5 * mm(pooled, b0_ref[0]))
        mz_out[...] = mz
        rims = mm(pick_ref[...], mz.astype(BF)).astype(BF)
        for d in range(4):
            rim_outs[d][...] = rims[16 * d:16 * d + 16]
        for copy in ahead:
            copy.wait()


def edge(rt, rim, mask, pw, bw, mid, pick, fine):
    whole = lambda *shape: pl.BlockSpec(shape, lambda b, i: (0,) * len(shape))
    return pl.pallas_call(
        edge_kernel,
        name="edge",
        grid=(2, 32 // RB),
        in_specs=[
            VM,
        ]
        + [pl.BlockSpec((1, 32, D), lambda b, i: (b, 0, 0))] * 2
        + [pl.BlockSpec((1, 34, D), lambda b, i: (b, 0, 0))] * 2
        + [
            pl.BlockSpec((RB, 32, 8), lambda b, i: (i, 0, 0)),
            whole(1, 4, D, D),
            whole(1, D, D),
            whole(2, 8, 8, D),
            whole(64, 128),
            pl.BlockSpec((1, RB, 32, D), lambda b, i: (b, i, 0, 0)),
            ANY,
            ANY,
        ],
        out_specs=[
            pl.BlockSpec((1, RB, 32, D), lambda b, i: (b, i, 0, 0)),
            pl.BlockSpec((1, RB, 32, D), lambda b, i: (b, i, 0, 0)),
            whole(128, D),
        ]
        + [whole(16, D)] * 4
        + [pl.BlockSpec(memory_space=pltpu.VMEM)] * 4,
        out_shape=[
            jax.ShapeDtypeStruct((2, 32, 32, D), BF),
            pltpu.HBM((2, 32, 32, D), F32),
            jax.ShapeDtypeStruct((128, D), F32),
        ]
        + [jax.ShapeDtypeStruct((16, D), BF)] * 4
        + [
            pltpu.VMEM((4, D, D), BF),
            pltpu.VMEM((4, D, D), BF),
            pltpu.VMEM((D, D), BF),
            pltpu.VMEM((2, D, D), BF),
        ],
        scratch_shapes=[
            pltpu.VMEM((3, 34, 32, D), BF),
            pltpu.VMEM((4, 40, D), F32),
            pltpu.VMEM((8, 4, 32, 128), F32),
            pltpu.VMEM((2, 8, 8, D), F32),
            pltpu.VMEM((8 * RB * 32, D), BF),
            pltpu.VMEM((D, D), BF),
            pltpu.SemaphoreType.DMA((4,)),
        ],
        compiler_params=pltpu.CompilerParams(vmem_limit_bytes=EDGE_VMEM << 20),
        cost_estimate=pl.CostEstimate(flops=2 * 8 * 2048 * D * D, bytes_accessed=16 << 20, transcendentals=16 << 20),
    )(rt, *rim, mask, pw, bw, mid, pick, fine, pw, bw)


def live_sides(first, last):
    at, count = lax.axis_index("lat"), lax.axis_size("lat")
    up = jnp.where(at > 0, 1.0, 0.0).astype(F32)
    down = jnp.where(at < count - 1, 1.0, 0.0).astype(F32)
    return jnp.where(first, up, 1.0), jnp.where(last, down, 1.0)


def middle_kernel(mz_ref, *refs):
    rim_refs = refs[:4]
    w_ref, c_ref, b1_ref, coarse_ref, gather_ref, mean_ref, mo_out, cz_out, czb_out, flat = refs[4:]
    for n in range(4):
        flat[2 * n:2 * n + 2, :] = coarse_ref[n // 2, n % 2]
    mz = mz_ref[...]
    own = mz.astype(BF)
    recv = 0.5 * (mm(own, w_ref[0]) + c_ref[1:2, :])
    states = jnp.concatenate([own] + [ref[...] for ref in rim_refs], axis=0)
    send = (0.5 * mm(states, w_ref[1])).astype(BF)
    near = mm(gather_ref[...], send)
    hidden = gate(near.reshape(8, 128, D) + recv[None]).astype(BF).reshape(1024, D)
    msg = gate(0.5 * mm(hidden, w_ref[2])).reshape(8, 128, D)
    lat = (lax.broadcasted_iota(jnp.int32, (128, D), 0) // 8) % 8
    up, down = live_sides(lat == 0, lat == 7)
    total = up * (msg[0] + msg[1] + msg[2]) + (msg[3] + msg[4]) + down * (msg[5] + msg[6] + msg[7])
    avg = (0.125 * total).astype(BF)
    mo = mz + mm(avg, w_ref[3])
    mo_out[...] = mo
    pooled = jnp.dot(mean_ref[...], mo, preferred_element_type=F32, precision=lax.Precision.HIGHEST)
    cz = flat[...] + gate(0.5 * mm(pooled.astype(BF), b1_ref[...]))
    cz_out[...] = cz
    czb_out[...] = cz.astype(BF)


VM = pl.BlockSpec(memory_space=pltpu.VMEM)


def full(*shape):
    return pl.BlockSpec(shape, lambda i: (0,) * len(shape))


def middle(mz, rim, pw, pb, bw, coarse, gather, mean):
    return pl.pallas_call(
        middle_kernel,
        name="middle",
        grid=(1,),
        in_specs=[full(128, D)]
        + [full(16, D)] * 2
        + [full(48, D)] * 2
        + [VM, full(3, D), VM, full(2, 2, 2, D), full(1024, 256), full(8, 128)],
        out_specs=[full(128, D), full(8, D), full(8, D)],
        out_shape=[
            jax.ShapeDtypeStruct((128, D), F32),
            jax.ShapeDtypeStruct((8, D), F32),
            jax.ShapeDtypeStruct((8, D), BF),
        ],
        scratch_shapes=[pltpu.VMEM((8, D), F32)],
        compiler_params=pltpu.CompilerParams(vmem_limit_bytes=24 << 20),
        cost_estimate=pl.CostEstimate(flops=2 * 12 * 128 * D * D, bytes_accessed=5 << 20, transcendentals=1 << 20),
    )(mz, *rim, pw, pb, bw, coarse, gather, mean)


def coarse_kernel(cz_ref, *refs):
    rim_refs = refs[:4]
    w_ref, c_ref, b23_ref, mo_ref, gather_ref, lift_ref, one_hbm, out_hbm, buf, sems = refs[4:]
    loads = []
    for n in range(8):
        at = (n // 4, pl.ds(8 * (n % 4), 8))
        loads.append(pltpu.make_async_copy(one_hbm.at[at], buf.at[n], sems.at[n, 0]))
        loads[-1].start()
    cz = cz_ref[...]
    own = cz.astype(BF)
    recv = 0.5 * (mm(own, w_ref[0]) + c_ref[2:3, :])
    pieces = [cz] + [ref[...].astype(F32) for ref in rim_refs] + [jnp.zeros((56, D), F32)]
    send = (0.5 * mm(jnp.concatenate(pieces, axis=0).astype(BF), w_ref[1])).astype(BF)
    near = mm(gather_ref[...], send)
    hidden = gate(near.reshape(8, 8, D) + recv[None]).astype(BF).reshape(64, D)
    msg = gate(0.5 * mm(hidden, w_ref[2])).reshape(8, 8, D)
    lat = (lax.broadcasted_iota(jnp.int32, (8, D), 0) // 2) % 2
    up, down = live_sides(lat == 0, lat == 1)
    total = up * (msg[0] + msg[1] + msg[2]) + (msg[3] + msg[4]) + down * (msg[5] + msg[6] + msg[7])
    avg = (0.125 * total).astype(BF)
    co = cz + mm(avg, w_ref[3])
    lifted = gate(0.5 * mm(co.astype(BF), b23_ref[0]))
    high = lifted.astype(BF).astype(F32)
    both = jnp.concatenate([high, lifted - high], axis=0).astype(BF)
    two = mo_ref[...] + mm(lift_ref[...], both)
    spread = gate(0.5 * mm(two.astype(BF), b23_ref[1])).reshape(16, 8, D)
    first = lax.broadcasted_iota(jnp.int32, (8, D), 0) < 4
    copies = []
    for n in range(8):
        loads[n].wait()
        for g in range(2):
            parts = []
            for t in range(4):
                low = jnp.broadcast_to(spread[2 * n + g, 2 * t:2 * t + 1, :], (8, D))
                high = jnp.broadcast_to(spread[2 * n + g, 2 * t + 1:2 * t + 2, :], (8, D))
                parts.append(jnp.where(first, low, high))
            wide = jnp.concatenate(parts, axis=0)
            for i in range(4 * g, 4 * g + 4):
                buf[n, i] = buf[n, i] + wide
        copies.append(pltpu.make_async_copy(buf.at[n], out_hbm.at[n // 4, pl.ds(8 * (n % 4), 8)], sems.at[n, 1]))
        copies[-1].start()
    for copy in copies:
        copy.wait()


def coarsest(cz, rim, pw, pb, bw, mo, gather, lift, one):
    return pl.pallas_call(
        coarse_kernel,
        name="coarsest",
        grid=(1,),
        in_specs=[full(8, D)]
        + [full(8, D)] * 2
        + [full(24, D)] * 2
        + [VM, full(3, D), VM, full(128, D), full(64, 128), full(128, 16), ANY],
        out_specs=ANY,
        out_shape=jax.ShapeDtypeStruct((2, 32, 32, D), F32),
        scratch_shapes=[pltpu.VMEM((8, 8, 32, D), F32), pltpu.SemaphoreType.DMA((8, 2))],
        compiler_params=pltpu.CompilerParams(vmem_limit_bytes=24 << 20),
        cost_estimate=pl.CostEstimate(flops=2 * 2 * 128 * D * D, bytes_accessed=4 << 20, transcendentals=1 << 18),
    )(cz, *rim, pw, pb, bw, mo, gather, lift, one)


def place_middle():
    pick = np.zeros((64, 128), np.float32)
    for b in range(2):
        for n in range(8):
            for d, (i, j) in enumerate(((0, n), (7, n), (n, 0), (n, 7))):
                pick[16 * d + 8 * b + n, 64 * b + 8 * i + j] = 1
    gather = np.zeros((1024, 256), np.float32)
    for k, (p, q) in enumerate(OFFS):
        for b in range(2):
            for i in range(8):
                for j in range(8):
                    y, x = i + p, j + q
                    if 0 <= x < 8:
                        n = 128 + 8 * b + x if y < 0 else 144 + 8 * b + x if y > 7 else 64 * b + 8 * y + x
                    else:
                        base = 160 + 8 * b if x < 0 else 208 + 8 * b
                        n = base + 16 + x % 8 if y < 0 else base + 32 + x % 8 if y > 7 else base + y
                    gather[128 * k + 64 * b + 8 * i + j, n] = 1
    mean = np.zeros((8, 128), np.float32)
    for b in range(2):
        for i in range(8):
            for j in range(8):
                mean[4 * b + 2 * (i // 4) + j // 4, 64 * b + 8 * i + j] = 1 / 16
    return pick, gather, mean


def place_coarse():
    gather = np.zeros((64, 128), np.float32)
    for k, (p, q) in enumerate(OFFS):
        for b in range(2):
            for i in range(2):
                for j in range(2):
                    y, x = i + p, j + q
                    base = (24 if x < 0 else 48 if x > 1 else 0) + (8 if y < 0 else 16 if y > 1 else 0)
                    gather[8 * k + 4 * b + 2 * i + j, base + 4 * b + 2 * (y % 2) + x % 2] = 1
    lift = np.zeros((128, 16), np.float32)
    for b in range(2):
        for i in range(8):
            for j in range(8):
                source = 4 * b + 2 * (i // 4) + j // 4
                lift[64 * b + 8 * i + j, source] = 1
                lift[64 * b + 8 * i + j, 8 + source] = 1
    return gather, lift


def trade(low_side, high_side, axis):
    count = lax.axis_size(axis)
    forward = [(i, (i + 1) % count) for i in range(count)]
    backward = [(i, (i - 1) % count) for i in range(count)]
    return lax.ppermute(high_side, axis, forward), lax.ppermute(low_side, axis, backward)


def local(fine, mid, coarse, flags, pw, bw, pb):
    fine, pw, bw = (pltpu.with_memory_space_constraint(a, pltpu.HBM) for a in (fine, pw, bw))
    top, bottom = rims(rows_kernel, (2, 1, 32, D), (0, 0, 0, 0), (0, 31, 0, 0), fine)
    up, down = trade(top, bottom, "lat")
    west, east = rims(columns_kernel, (2, 32, 8, D), (0, 0, 0, 0), (0, 0, 3, 0), fine)
    left, right = trade(
        jnp.concatenate([west, up[:, :1], down[:, :1]], axis=1),
        jnp.concatenate([east, up[:, 31:], down[:, 31:]], axis=1),
        "lon",
    )
    lat = lax.axis_index("lat")
    rows = lax.axis_size("lat")
    index = jnp.arange(32)
    step = jnp.asarray([p for p, q in OFFS])[:, None]
    where = lat * 32 + index[None, :] + step
    live = flags.astype(F32) * ((where >= 0) & (where < rows * 32)).astype(F32)[:, :, None]
    mask = jnp.transpose(live, (1, 2, 0))
    pick, gather, mean = place_middle()
    gather_c, lift = place_coarse()
    rt = prep(fine, pw, pb)
    avg, one, mz, top, bottom, west, east, w1, w2, b1, b23 = edge(
        rt, (up, down, left, right), mask, pw, bw, mid, jnp.asarray(pick, BF), fine
    )
    one = pltpu.with_memory_space_constraint(one, pltpu.HBM)
    up, down = trade(top, bottom, "lat")
    left, right = trade(jnp.concatenate([west, up, down]), jnp.concatenate([east, up, down]), "lon")
    mo, cz, czb = middle(
        mz, (up, down, left, right), w1, pb, b1, coarse, jnp.asarray(gather, BF), jnp.asarray(mean, F32)
    )
    up, down = trade(czb, czb, "lat")
    column = jnp.concatenate([czb, up, down])
    left, right = trade(column, column, "lon")
    refined = coarsest(
        cz, (up, down, left, right), w2, pb, b23, mo, jnp.asarray(gather_c, BF), jnp.asarray(lift, BF), one
    )
    return refined, avg


def solution(mesh):
    node = P(None, "lat", "lon", None)
    return jax.shard_map(
        local,
        mesh=mesh,
        in_specs=(node, node, node, P(None, "lat", "lon"), P(), P(), P()),
        out_specs=(node, node),
        check_vma=False,
    )
```

```python
import functools
import jax
import jax.numpy as jnp
import numpy as np
from jax import lax
from jax.experimental import pallas as pl
from jax.experimental.pallas import tpu as pltpu
from jax.sharding import PartitionSpec as P

D = 512
ANY = pl.BlockSpec(memory_space=pl.ANY)
VM = pl.BlockSpec(memory_space=pltpu.VMEM)
BF = jnp.bfloat16
F32 = jnp.float32
OFFS = ((-1, -1), (-1, 0), (-1, 1), (0, -1), (0, 1), (1, -1), (1, 0), (1, 1))
PRB = 8
EDGE_VMEM = 28
RB = 8
EDGE_VMEM = 28


def mm(a, b):
    return jnp.dot(a, b, preferred_element_type=F32)


def gate(half):
    return half + half * jnp.tanh(half)


def pool_rows(x, g, tmp):
    tall = (x[4 * g] + x[4 * g + 1]) + (x[4 * g + 2] + x[4 * g + 3])
    parts = []
    for lane in range(4):
        tmp[g, lane] = tall[:, lane * 128:(lane + 1) * 128]
        part = tmp[g, lane, pl.ds(0, 8, stride=4), :]
        for t in range(1, 4):
            part = part + tmp[g, lane, pl.ds(t, 8, stride=4), :]
        parts.append(part)
    return jnp.concatenate(parts, axis=1)


def rows_kernel(top_ref, bottom_ref, top_out, bottom_out):
    top_out[...] = top_ref[...].reshape(2, 32, D).astype(BF)
    bottom_out[...] = bottom_ref[...].reshape(2, 32, D).astype(BF)


def columns_kernel(west_ref, east_ref, west_out, east_out):
    for b in range(2):
        west_out[b] = west_ref[b, :, 0, :].astype(BF)
        east_out[b] = east_ref[b, :, 7, :].astype(BF)


def rims(body, shape, first, last, fine):
    out = pl.BlockSpec((2, 32, D), lambda i: (0, 0, 0))
    return pl.pallas_call(
        body,
        name=body.__name__,
        grid=(1,),
        in_specs=[pl.BlockSpec(shape, lambda i: first), pl.BlockSpec(shape, lambda i: last)],
        out_specs=[out] * 2,
        out_shape=[jax.ShapeDtypeStruct((2, 32, D), BF)] * 2,
        compiler_params=pltpu.CompilerParams(vmem_limit_bytes=24 << 20),
        cost_estimate=pl.CostEstimate(flops=1 << 24, bytes_accessed=3 << 20, transcendentals=0),
    )(fine, fine)


def prep_kernel(s_hbm, w_hbm, c_ref, rt_out, s_ref, w_ref, sems, w_sem):
    weights = pltpu.make_async_copy(w_hbm.at[0, 0:2], w_ref, w_sem)
    weights.start()
    copies = []
    for n in range(4):
        at = (n // 2, pl.ds(16 * (n % 2), 16))
        copies.append(pltpu.make_async_copy(s_hbm.at[at], s_ref.at[n], sems.at[n]))
        copies[-1].start()
    weights.wait()
    for n in range(4):
        copies[n].wait()
        b, i = n // 2, n % 2
        x = s_ref[n]
        op = x.reshape(512, D).astype(BF)
        rt_out[0, b, 16 * i:16 * i + 16] = (0.5 * (mm(op, w_ref[0]) + c_ref[0:1, :])).astype(BF).reshape(16, 32, D)
        rt_out[1, b, 16 * i:16 * i + 16] = (0.5 * mm(op, w_ref[1])).astype(BF).reshape(16, 32, D)


def prep(fine, pw, pb):
    full4 = lambda *shape: pl.BlockSpec(shape, lambda i: (0,) * len(shape))
    return pl.pallas_call(
        prep_kernel,
        name="prep",
        grid=(1,),
        in_specs=[ANY, ANY, full4(3, D)],
        out_specs=full4(2, 2, 32, 32, D),
        out_shape=pltpu.VMEM((2, 2, 32, 32, D), BF),
        scratch_shapes=[
            pltpu.VMEM((4, 16, 32, D), F32),
            pltpu.VMEM((2, D, D), BF),
            pltpu.SemaphoreType.DMA((4,)),
            pltpu.SemaphoreType.DMA,
        ],
        compiler_params=pltpu.CompilerParams(vmem_limit_bytes=24 << 20),
        cost_estimate=pl.CostEstimate(flops=2 * 2 * 2048 * D * D, bytes_accessed=5 << 20, transcendentals=0),
    )(fine, pw, pb)


def messages(rt_ref, live_ref, w_ref, s_ref, sh, w2_half, avg_out, one_out, hid, tmp, pa, blk):
    b, half = pl.program_id(0), pl.program_id(1)
    row0 = blk * RB
    span = RB * 32
    rv = rt_ref[0, b, pl.ds(row0, RB)].reshape(span, D)
    live = live_ref[...].reshape(span, 8)
    for k, (p, q) in enumerate(OFFS):
        sv = sh[b, q + 1, pl.ds(row0 + 1 + p, RB)].reshape(span, D)
        m = jnp.broadcast_to(live[:, k:k + 1], (span, 128)).astype(BF)
        hid[k * span:(k + 1) * span] = gate(rv + sv) * jnp.concatenate([m] * 4, axis=1)
    msg = gate(mm(hid[...], w2_half[...])).reshape(8, span, D)
    avg = (jnp.sum(msg, axis=0) * 0.125).astype(BF)
    avg_out[0] = avg.reshape(RB, 32, D)
    one = s_ref[0] + mm(avg, w_ref[0, 3]).reshape(RB, 32, D)
    one_out[0] = one
    for g in range(RB // 4):
        pa[b, half, g] = pool_rows(one, g, tmp)


def parents(pa, mid, b0_ref):
    pooled = (pa[...].reshape(64, D) * 0.0625).astype(BF)
    return mid.reshape(64, D) + gate(0.5 * mm(pooled, b0_ref[0]))


def outer_kernel(rt_ref, up_ref, down_ref, left_ref, right_ref, live_ref, w_ref, b0_ref, mid_ref, s_ref, pw_hbm, bw_hbm,
                 avg_out, one_out, mz_out, top_out, bottom_out, w1_out, w2_out, b1_out, b23_out, sh, w2_half,
                 hs, tmp, pa, hid, sems):
    b, half = pl.program_id(0), pl.program_id(1)
    ahead = [
        pltpu.make_async_copy(pw_hbm.at[1], w1_out, sems.at[0]),
        pltpu.make_async_copy(pw_hbm.at[2], w2_out, sems.at[1]),
        pltpu.make_async_copy(bw_hbm.at[1], b1_out, sems.at[2]),
        pltpu.make_async_copy(bw_hbm.at[2:4], b23_out, sems.at[3]),
    ]

    @pl.when((b == 0) & (half == 0))
    def _():
        for copy in ahead:
            copy.start()
        w2_half[...] = (w_ref[0, 2].astype(F32) * 0.5).astype(BF)

    @pl.when(half == 0)
    def _():
        for n, ref in enumerate((up_ref, down_ref, left_ref, right_ref)):
            hs[n, 0:ref.shape[1], :] = (0.5 * mm(ref[0], w_ref[0, 1])).astype(BF).astype(F32)
        rows = lax.broadcasted_iota(jnp.int32, (32, D), 0)

        def put(i, x, left, right):
            sh[b, 1, i] = x.astype(BF)
            sh[b, 0, i] = jnp.where(rows == 0, jnp.broadcast_to(left, (32, D)), pltpu.roll(x, 1, 0)).astype(BF)
            sh[b, 2, i] = jnp.where(rows == 31, jnp.broadcast_to(right, (32, D)), pltpu.roll(x, 31, 0)).astype(BF)

        put(0, hs[0, 0:32, :], hs[2, 32:33, :], hs[3, 32:33, :])
        put(33, hs[1, 0:32, :], hs[2, 33:34, :], hs[3, 33:34, :])

        @pl.loop(0, 32, unroll=4)
        def _(i):
            put(i + 1, rt_ref[1, b, i].astype(F32), hs[2, pl.ds(i, 1), :], hs[3, pl.ds(i, 1), :])

    messages(rt_ref, live_ref, w_ref, s_ref, sh, w2_half, avg_out, one_out, hid, tmp, pa, 3 * half)

    @pl.when((b == 1) & (half == 1))
    def _():
        mid = [mid_ref[n // 2, 6 * (n % 2):6 * (n % 2) + 2] for n in range(4)]
        mz = parents(pa, jnp.concatenate(mid, axis=0), b0_ref)
        mz_out[...] = mz
        top_out[...] = jnp.concatenate([mz[0:8], mz[32:40]], axis=0).astype(BF)
        bottom_out[...] = jnp.concatenate([mz[24:32], mz[56:64]], axis=0).astype(BF)
        for copy in ahead:
            copy.wait()


def inner_kernel(rt_ref, live_ref, w_ref, b0_ref, mid_ref, s_ref, sh, w2_half, mzo_ref, pick_ref, avg_in, one_in,
                 avg_out, one_out, mz_out, west_out, east_out, tmp, pa, hid):
    b, half = pl.program_id(0), pl.program_id(1)
    messages(rt_ref, live_ref, w_ref, s_ref, sh, w2_half, avg_out, one_out, hid, tmp, pa, half + 1)

    @pl.when((b == 1) & (half == 1))
    def _():
        mzi = parents(pa, mid_ref[:, 2:6], b0_ref)
        mzo = mzo_ref[...]
        mz = jnp.concatenate([mzo[0:16], mzi[0:32], mzo[16:48], mzi[32:64], mzo[48:64]], axis=0)
        mz_out[...] = mz
        sides = mm(pick_ref[...], mz.astype(BF)).astype(BF)
        west_out[...] = sides[0:16]
        east_out[...] = sides[16:32]


def edge_specs(place):
    whole = lambda *shape: pl.BlockSpec(shape, lambda b, i: (0,) * len(shape))
    tile = pl.BlockSpec((1, RB, 32, D), lambda b, i: (b, place(i), 0, 0))
    live = pl.BlockSpec((RB, 32, 8), lambda b, i: (place(i), 0, 0))
    return whole, tile, live


EDGE = dict(
    compiler_params=pltpu.CompilerParams(vmem_limit_bytes=EDGE_VMEM << 20),
    cost_estimate=pl.CostEstimate(flops=8 * 2048 * D * D, bytes_accessed=8 << 20, transcendentals=8 << 20),
)
SCRATCH = [
    pltpu.VMEM((8, 4, 32, 128), F32),
    pltpu.VMEM((2, 2, 2, 8, D), F32),
    pltpu.VMEM((8 * RB * 32, D), BF),
]
SHARED = [pltpu.HBM((2, 32, 32, D), BF), pltpu.HBM((2, 32, 32, D), F32)]


def outer(rt, rim, mask, pw, bw, mid, fine):
    whole, tile, live = edge_specs(lambda i: 3 * i)
    return pl.pallas_call(
        outer_kernel,
        name="outer",
        grid=(2, 2),
        in_specs=[VM]
        + [pl.BlockSpec((1, 32, D), lambda b, i: (b, 0, 0))] * 2
        + [pl.BlockSpec((1, 34, D), lambda b, i: (b, 0, 0))] * 2
        + [live, whole(1, 4, D, D), whole(1, D, D), whole(2, 8, 8, D), tile, ANY, ANY],
        out_specs=[tile, tile, whole(64, D), whole(16, D), whole(16, D)] + [VM] * 6,
        out_shape=SHARED
        + [
            jax.ShapeDtypeStruct((64, D), F32),
            jax.ShapeDtypeStruct((16, D), BF),
            jax.ShapeDtypeStruct((16, D), BF),
            pltpu.VMEM((4, D, D), BF),
            pltpu.VMEM((4, D, D), BF),
            pltpu.VMEM((D, D), BF),
            pltpu.VMEM((2, D, D), BF),
            pltpu.VMEM((2, 3, 34, 32, D), BF),
            pltpu.VMEM((D, D), BF),
        ],
        scratch_shapes=[pltpu.VMEM((4, 40, D), F32)] + SCRATCH + [pltpu.SemaphoreType.DMA((4,))],
        **EDGE,
    )(rt, *rim, mask, pw, bw, mid, fine, pw, bw)


def inner(rt, mask, pw, bw, mid, fine, sh, w2_half, mzo, pick, avg, one):
    whole, tile, live = edge_specs(lambda i: i + 1)
    return pl.pallas_call(
        inner_kernel,
        name="inner",
        grid=(2, 2),
        in_specs=[VM, live, whole(1, 4, D, D), whole(1, D, D), whole(2, 8, 8, D), tile, VM, VM]
        + [whole(64, D), whole(32, 128), ANY, ANY],
        out_specs=[tile, tile, whole(128, D), whole(16, D), whole(16, D)],
        out_shape=SHARED
        + [
            jax.ShapeDtypeStruct((128, D), F32),
            jax.ShapeDtypeStruct((16, D), BF),
            jax.ShapeDtypeStruct((16, D), BF),
        ],
        input_output_aliases={10: 0, 11: 1},
        scratch_shapes=SCRATCH,
        **EDGE,
    )(rt, mask, pw, bw, mid, fine, sh, w2_half, mzo, pick, avg, one)


def live_sides(first, last):
    at, count = lax.axis_index("lat"), lax.axis_size("lat")
    up = jnp.where(at > 0, 1.0, 0.0).astype(F32)
    down = jnp.where(at < count - 1, 1.0, 0.0).astype(F32)
    return jnp.where(first, up, 1.0), jnp.where(last, down, 1.0)


def middle_kernel(mz_ref, *refs):
    rim_refs = refs[:4]
    w_ref, c_ref, b1_ref, coarse_ref, gather_ref, mean_ref, mo_out, cz_out, czb_out, flat = refs[4:]
    for n in range(4):
        flat[2 * n:2 * n + 2, :] = coarse_ref[n // 2, n % 2]
    mz = mz_ref[...]
    own = mz.astype(BF)
    recv = 0.5 * (mm(own, w_ref[0]) + c_ref[1:2, :])
    states = jnp.concatenate([own] + [ref[...] for ref in rim_refs], axis=0)
    send = (0.5 * mm(states, w_ref[1])).astype(BF)
    near = mm(gather_ref[...], send)
    hidden = gate(near.reshape(8, 128, D) + recv[None]).astype(BF).reshape(1024, D)
    msg = gate(0.5 * mm(hidden, w_ref[2])).reshape(8, 128, D)
    lat = (lax.broadcasted_iota(jnp.int32, (128, D), 0) // 8) % 8
    up, down = live_sides(lat == 0, lat == 7)
    total = up * (msg[0] + msg[1] + msg[2]) + (msg[3] + msg[4]) + down * (msg[5] + msg[6] + msg[7])
    avg = (0.125 * total).astype(BF)
    mo = mz + mm(avg, w_ref[3])
    mo_out[...] = mo
    pooled = jnp.dot(mean_ref[...], mo, preferred_element_type=F32, precision=lax.Precision.HIGHEST)
    cz = flat[...] + gate(0.5 * mm(pooled.astype(BF), b1_ref[...]))
    cz_out[...] = cz
    czb_out[...] = cz.astype(BF)


def full(*shape):
    return pl.BlockSpec(shape, lambda i: (0,) * len(shape))


def middle(mz, rim, pw, pb, bw, coarse, gather, mean):
    return pl.pallas_call(
        middle_kernel,
        name="middle",
        grid=(1,),
        in_specs=[full(128, D)]
        + [full(16, D)] * 2
        + [full(48, D)] * 2
        + [VM, full(3, D), VM, full(2, 2, 2, D), full(1024, 256), full(8, 128)],
        out_specs=[full(128, D), full(8, D), full(8, D)],
        out_shape=[
            jax.ShapeDtypeStruct((128, D), F32),
            jax.ShapeDtypeStruct((8, D), F32),
            jax.ShapeDtypeStruct((8, D), BF),
        ],
        scratch_shapes=[pltpu.VMEM((8, D), F32)],
        compiler_params=pltpu.CompilerParams(vmem_limit_bytes=24 << 20),
        cost_estimate=pl.CostEstimate(flops=2 * 12 * 128 * D * D, bytes_accessed=5 << 20, transcendentals=1 << 20),
    )(mz, *rim, pw, pb, bw, coarse, gather, mean)


def coarse_kernel(cz_ref, *refs):
    rim_refs = refs[:4]
    w_ref, c_ref, b23_ref, mo_ref, gather_ref, lift_ref, one_hbm, out_hbm, buf, sems = refs[4:]
    loads = []
    for n in range(8):
        at = (n // 4, pl.ds(8 * (n % 4), 8))
        loads.append(pltpu.make_async_copy(one_hbm.at[at], buf.at[n], sems.at[n, 0]))
        loads[-1].start()
    cz = cz_ref[...]
    own = cz.astype(BF)
    recv = 0.5 * (mm(own, w_ref[0]) + c_ref[2:3, :])
    pieces = [cz] + [ref[...].astype(F32) for ref in rim_refs] + [jnp.zeros((56, D), F32)]
    send = (0.5 * mm(jnp.concatenate(pieces, axis=0).astype(BF), w_ref[1])).astype(BF)
    near = mm(gather_ref[...], send)
    hidden = gate(near.reshape(8, 8, D) + recv[None]).astype(BF).reshape(64, D)
    msg = gate(0.5 * mm(hidden, w_ref[2])).reshape(8, 8, D)
    lat = (lax.broadcasted_iota(jnp.int32, (8, D), 0) // 2) % 2
    up, down = live_sides(lat == 0, lat == 1)
    total = up * (msg[0] + msg[1] + msg[2]) + (msg[3] + msg[4]) + down * (msg[5] + msg[6] + msg[7])
    avg = (0.125 * total).astype(BF)
    co = cz + mm(avg, w_ref[3])
    lifted = gate(0.5 * mm(co.astype(BF), b23_ref[0]))
    high = lifted.astype(BF).astype(F32)
    both = jnp.concatenate([high, lifted - high], axis=0).astype(BF)
    two = mo_ref[...] + mm(lift_ref[...], both)
    spread = gate(0.5 * mm(two.astype(BF), b23_ref[1])).reshape(16, 8, D)
    first = lax.broadcasted_iota(jnp.int32, (8, D), 0) < 4
    copies = []
    for n in range(8):
        loads[n].wait()
        for g in range(2):
            parts = []
            for t in range(4):
                low = jnp.broadcast_to(spread[2 * n + g, 2 * t:2 * t + 1, :], (8, D))
                high = jnp.broadcast_to(spread[2 * n + g, 2 * t + 1:2 * t + 2, :], (8, D))
                parts.append(jnp.where(first, low, high))
            wide = jnp.concatenate(parts, axis=0)
            for i in range(4 * g, 4 * g + 4):
                buf[n, i] = buf[n, i] + wide
        copies.append(pltpu.make_async_copy(buf.at[n], out_hbm.at[n // 4, pl.ds(8 * (n % 4), 8)], sems.at[n, 1]))
        copies[-1].start()
    for copy in copies:
        copy.wait()


def coarsest(cz, rim, pw, pb, bw, mo, gather, lift, one):
    return pl.pallas_call(
        coarse_kernel,
        name="coarsest",
        grid=(1,),
        in_specs=[full(8, D)]
        + [full(8, D)] * 2
        + [full(24, D)] * 2
        + [VM, full(3, D), VM, full(128, D), full(64, 128), full(128, 16), ANY],
        out_specs=ANY,
        out_shape=jax.ShapeDtypeStruct((2, 32, 32, D), F32),
        scratch_shapes=[pltpu.VMEM((8, 8, 32, D), F32), pltpu.SemaphoreType.DMA((8, 2))],
        compiler_params=pltpu.CompilerParams(vmem_limit_bytes=24 << 20),
        cost_estimate=pl.CostEstimate(flops=2 * 2 * 128 * D * D, bytes_accessed=4 << 20, transcendentals=1 << 18),
    )(cz, *rim, pw, pb, bw, mo, gather, lift, one)


def place_middle():
    pick = np.zeros((32, 128), np.float32)
    for b in range(2):
        for n in range(8):
            for d, (i, j) in enumerate(((n, 0), (n, 7))):
                pick[16 * d + 8 * b + n, 64 * b + 8 * i + j] = 1
    gather = np.zeros((1024, 256), np.float32)
    for k, (p, q) in enumerate(OFFS):
        for b in range(2):
            for i in range(8):
                for j in range(8):
                    y, x = i + p, j + q
                    if 0 <= x < 8:
                        n = 128 + 8 * b + x if y < 0 else 144 + 8 * b + x if y > 7 else 64 * b + 8 * y + x
                    else:
                        base = 160 + 8 * b if x < 0 else 208 + 8 * b
                        n = base + 16 + x % 8 if y < 0 else base + 32 + x % 8 if y > 7 else base + y
                    gather[128 * k + 64 * b + 8 * i + j, n] = 1
    mean = np.zeros((8, 128), np.float32)
    for b in range(2):
        for i in range(8):
            for j in range(8):
                mean[4 * b + 2 * (i // 4) + j // 4, 64 * b + 8 * i + j] = 1 / 16
    return pick, gather, mean


def place_coarse():
    gather = np.zeros((64, 128), np.float32)
    for k, (p, q) in enumerate(OFFS):
        for b in range(2):
            for i in range(2):
                for j in range(2):
                    y, x = i + p, j + q
                    base = (24 if x < 0 else 48 if x > 1 else 0) + (8 if y < 0 else 16 if y > 1 else 0)
                    gather[8 * k + 4 * b + 2 * i + j, base + 4 * b + 2 * (y % 2) + x % 2] = 1
    lift = np.zeros((128, 16), np.float32)
    for b in range(2):
        for i in range(8):
            for j in range(8):
                source = 4 * b + 2 * (i // 4) + j // 4
                lift[64 * b + 8 * i + j, source] = 1
                lift[64 * b + 8 * i + j, 8 + source] = 1
    return gather, lift


def trade(low_side, high_side, axis):
    count = lax.axis_size(axis)
    forward = [(i, (i + 1) % count) for i in range(count)]
    backward = [(i, (i - 1) % count) for i in range(count)]
    return lax.ppermute(high_side, axis, forward), lax.ppermute(low_side, axis, backward)


def local(fine, mid, coarse, flags, pw, bw, pb):
    fine, pw, bw = (pltpu.with_memory_space_constraint(a, pltpu.HBM) for a in (fine, pw, bw))
    top, bottom = rims(rows_kernel, (2, 1, 32, D), (0, 0, 0, 0), (0, 31, 0, 0), fine)
    up, down = trade(top, bottom, "lat")
    west, east = rims(columns_kernel, (2, 32, 8, D), (0, 0, 0, 0), (0, 0, 3, 0), fine)
    left, right = trade(
        jnp.concatenate([west, up[:, :1], down[:, :1]], axis=1),
        jnp.concatenate([east, up[:, 31:], down[:, 31:]], axis=1),
        "lon",
    )
    lat = lax.axis_index("lat")
    rows = lax.axis_size("lat")
    index = jnp.arange(32)
    step = jnp.asarray([p for p, q in OFFS])[:, None]
    where = lat * 32 + index[None, :] + step
    live = flags.astype(F32) * ((where >= 0) & (where < rows * 32)).astype(F32)[:, :, None]
    mask = jnp.transpose(live, (1, 2, 0))
    pick, gather, mean = place_middle()
    gather_c, lift = place_coarse()
    rt = prep(fine, pw, pb)
    avg, one, mzo, top, bottom, w1, w2, b1, b23, sh, w2_half = outer(rt, (up, down, left, right), mask, pw, bw, mid, fine)
    up, down = trade(top, bottom, "lat")
    avg, one, mz, west, east = inner(rt, mask, pw, bw, mid, fine, sh, w2_half, mzo, jnp.asarray(pick, BF), avg, one)
    one = pltpu.with_memory_space_constraint(one, pltpu.HBM)
    left, right = trade(jnp.concatenate([west, up, down]), jnp.concatenate([east, up, down]), "lon")
    mo, cz, czb = middle(
        mz, (up, down, left, right), w1, pb, b1, coarse, jnp.asarray(gather, BF), jnp.asarray(mean, F32)
    )
    up, down = trade(czb, czb, "lat")
    column = jnp.concatenate([czb, up, down])
    left, right = trade(column, column, "lon")
    refined = coarsest(
        cz, (up, down, left, right), w2, pb, b23, mo, jnp.asarray(gather_c, BF), jnp.asarray(lift, BF), one
    )
    return refined, avg


def solution(mesh):
    node = P(None, "lat", "lon", None)
    return jax.shard_map(
        local,
        mesh=mesh,
        in_specs=(node, node, node, P(None, "lat", "lon"), P(), P(), P()),
        out_specs=(node, node),
        check_vma=False,
    )
```
